128 devices in a mesh: dp: 8 (over y, core), tp: 16 (over z, x).
Axes of the slice: x: 4, y: 4, z: 4, core: 2. Of those that a mesh axis runs over, the one named last changes fastest.
Arguments:
- tokens: bfloat16 [10240, 6144], P(('dp', 'tp')), parts along dimension 0, may hold values from -6 to 6
- ln_gain: float32 [6144], replicated, may hold values from 0.25 to 1.75
- ln_bias: float32 [6144], replicated, may hold values from -1.75 to 1.75
- w_qkv: bfloat16 [6144, 3, 6144], P(None, None, 'tp'), may hold values from -0.45927933 to 0.45927933
- b_qkv: float32 [3, 6144], P(None, 'tp'), may hold values from -3 to 3
- w_out: bfloat16 [6144, 6144], P('tp'), may hold values from -0.078125 to 0.078125
- b_out: float32 [6144], replicated, may hold values from -1.25 to 1.25
- kv_cache: bfloat16 [2, 96, 128, 6144], P(None, 'dp', None, 'tp'), parts along dimension 1, may hold values from -6 to 6
- page_table: int32 [8, 10], P('dp'), parts along dimension 0, may hold values from 0 to 11, as said below
- lengths: int32 [8], P('dp'), parts along dimension 0, may hold values from 641 to 1280
Outputs:
- attn_out: bfloat16 [10240, 6144], P(('dp', 'tp')), parts along dimension 0
- kv_cache_out: bfloat16 [2, 96, 128, 6144], P(None, 'dp', None, 'tp'), parts along dimension 1
The draws below stay inside these ranges and needn't reach their ends.
There are 8 independent parts, one for each index of `dp`. The reference program is written for one: setup_inputs(seed, part) draws one part's arguments, and reference() takes and returns one part's arrays. A program takes and returns all parts, laid end to end along the dimension named above; an argument that names none is the same for every part. Nothing has to cross between parts.
Inputs may be any that keep to these rules, and one draw needn't show every extreme that they name: `page_table`: no slot is named twice within a part.
All inputs are finite; a program needn't handle non-finite values.
Results may differ from the reference program's by a relative error of at most 0.015.
The reference program's roundings to bfloat16 on the way (of `normed`, `projected`, `weights` and `attended`) count: a program that leaves them out, or rounds other values in their place, can miss the bound.
Values may be sent and summed in bfloat16 or wider, within the bound.
A program may use at most 128 MiB of HBM per device.

```python
import math
import jax
import jax.numpy as jnp
from jax import lax

D = 6144
HEADS = 48
HD = 128
SEQS = 1
PAGE = 128
FEAT = 6144
TOKENS = 1280
LEN = 1280
PAGES = 10
SLOTS = 12


def draw_w_qkv(key, part):
    normal_part = jnp.clip(jax.random.normal(jax.random.fold_in(key, 5), (D, 3, FEAT), jnp.float32), -6.0, 6.0) * (1.0 / math.sqrt(D))
    return normal_part.astype(jnp.bfloat16)


def draw_page_table(key, part):
    shuffled = jax.random.permutation(jax.random.fold_in(key, 11), SLOTS)
    return shuffled[:SEQS * PAGES].reshape(SEQS, PAGES).astype(jnp.int32)


def block_levels(rng, shape, pieces, low, top_value):
    level = 1.0
    for position, blocks in pieces:
        heights = jax.random.uniform(jax.random.fold_in(jax.random.fold_in(rng, 6), position), (blocks,), jnp.float32, low / len(pieces), top_value / len(pieces))
        level = level * jnp.repeat(jnp.exp(heights), shape[position] // blocks).reshape((-1,) + (1,) * (len(shape) - 1 - position))
    return level


def bell_draw(rng, dims, scale, most, shards=(), kind=jnp.bfloat16):
    drawn = jax.random.normal(rng, dims, jnp.float32) * scale
    if len(shards) > 0:
        drawn = block_levels(rng, dims, shards, -0.22, 0.18) * drawn
    return jnp.clip(drawn, min=-most, max=most).astype(kind)


def setup_inputs(seed: int = 0, part: int = 0) -> dict:
    arg_keys = jax.random.split(jax.random.key(seed), 11)
    own_keys = jax.random.split(jax.random.fold_in(arg_keys[10], part), 11)
    tokens = bell_draw(own_keys[0], (TOKENS, D), 1.0, 6.0, ((0, 16),))
    ln_gain = jnp.clip(1.0 + 0.15 * jax.random.normal(arg_keys[1], (D,), jnp.float32), 0.25, 1.75)
    ln_bias = bell_draw(arg_keys[2], (D,), 0.3, 1.75, (), jnp.float32)
    w_qkv = draw_w_qkv(jax.random.fold_in(arg_keys[10], 71), part)
    b_qkv = bell_draw(arg_keys[4], (3, FEAT), 0.5, 3.0, ((1, 16),), jnp.float32)
    w_out = bell_draw(arg_keys[5], (FEAT, D), FEAT ** -0.5, 0.078125, ((0, 16),))
    b_out = bell_draw(arg_keys[6], (D,), 0.2, 1.25, (), jnp.float32)
    kv_cache = bell_draw(own_keys[7], (2, SLOTS, PAGE, FEAT), 1.0, 6.0, ((3, 16),))
    page_table = draw_page_table(jax.random.fold_in(jax.random.fold_in(arg_keys[10], part), 71), part)
    lengths = jax.random.randint(own_keys[9], (SEQS,), LEN // 2 + 1, LEN + 1).astype(jnp.int32)
    return {"tokens": tokens, "ln_gain": ln_gain, "ln_bias": ln_bias, "w_qkv": w_qkv, "b_qkv": b_qkv, "w_out": w_out, "b_out": b_out, "kv_cache": kv_cache, "page_table": page_table, "lengths": lengths}


norm_eps = 1e-05

def layer_norm(token_rows, gain_row, shift_row):
    floats = token_rows.astype(jnp.float32)
    center = lax.optimization_barrier(jnp.mean(floats, axis=-1, keepdims=True))
    spread = lax.optimization_barrier(jnp.mean(jnp.square(floats - center), axis=-1, keepdims=True))
    return ((floats - center) * lax.rsqrt(spread + norm_eps) * gain_row + shift_row).astype(jnp.bfloat16)

def attend(queries, keys, values, lengths):
    seq_count, seq_len, head_count, head_dim = queries.shape
    block_len = math.gcd(seq_len, 512)
    score_scale = 1.0 / math.sqrt(head_dim)
    key_pos = jnp.arange(seq_len, dtype=jnp.int32)

    def one_sequence(inputs):
        seq_query, seq_key, seq_value, length = inputs
        blocks = seq_query.reshape(seq_len // block_len, block_len, head_count, head_dim)

        def one_block(block_pair):
            block_query, block_index = block_pair
            scores = jnp.einsum('qhe,khe->hqk', block_query.astype(jnp.float32), seq_key.astype(jnp.float32)) * score_scale
            query_pos = block_index * block_len + jnp.arange(block_len, dtype=jnp.int32)
            allowed = (key_pos[None, :] <= query_pos[:, None]) & (key_pos[None, :] < length)
            scores = jnp.where(allowed[None], scores, -1e+30)
            row_max = lax.optimization_barrier(jnp.max(scores, axis=-1, keepdims=True))
            raised = jnp.exp(scores - row_max)
            weights = (raised / lax.optimization_barrier(jnp.sum(raised, axis=-1, keepdims=True))).astype(jnp.bfloat16)
            return jnp.einsum('hqk,khe->qhe', weights.astype(jnp.float32), seq_value.astype(jnp.float32)).astype(jnp.bfloat16)
        results = lax.map(one_block, (blocks, jnp.arange(seq_len // block_len, dtype=jnp.int32)))
        return results.reshape(seq_len, head_count, head_dim)
    return lax.map(one_sequence, (queries, keys, values, lengths.astype(jnp.int32)))

def write_cache(kv_cache, key_value, page_table, lengths):
    seq_count, page_count = page_table.shape
    page_len = kv_cache.shape[2]
    feat_here = kv_cache.shape[3]
    fresh_pages = jnp.moveaxis(key_value, 1, 0).reshape(2, seq_count * page_count, page_len, feat_here)
    slot_ids = page_table.reshape(-1).astype(jnp.int32)
    positions = jnp.arange(page_count, dtype=jnp.int32)[:, None] * page_len + jnp.arange(page_len, dtype=jnp.int32)[None, :]
    written = (positions[None] < lengths.astype(jnp.int32)[:, None, None]).reshape(seq_count * page_count, page_len)
    current = kv_cache[:, slot_ids]
    new_pages = jnp.where(written[None, :, :, None], fresh_pages, current)
    return kv_cache.at[:, slot_ids].set(new_pages)

def reference(tokens, ln_gain, ln_bias, w_qkv, b_qkv, w_out, b_out, kv_cache, page_table, lengths):
    normed = layer_norm(tokens, ln_gain, ln_bias)
    flat = jnp.dot(normed, w_qkv.reshape(D, 3 * FEAT), preferred_element_type=jnp.float32) + b_qkv.reshape(-1)
    projected = flat.astype(jnp.bfloat16).reshape(TOKENS, 3, FEAT)
    queries = projected[:, 0].reshape(SEQS, LEN, HEADS, HD)
    keys = projected[:, 1].reshape(SEQS, LEN, HEADS, HD)
    values = projected[:, 2].reshape(SEQS, LEN, HEADS, HD)
    attended = attend(queries, keys, values, lengths).reshape(TOKENS, FEAT)
    attn_out = (jnp.dot(attended, w_out, preferred_element_type=jnp.float32) + b_out).astype(jnp.bfloat16)
    kv_cache_out = write_cache(kv_cache, projected[:, 1:3], page_table, lengths)
    return (attn_out, kv_cache_out)
```

```python
import functools

import jax
import jax.numpy as jnp
from jax import lax
from jax.experimental import pallas as pl
from jax.experimental.pallas import tpu as pltpu
from jax.sharding import PartitionSpec as P

HD = 128
EPS = 1e-05
MESH = pl.DeviceIdType.MESH
RINGS = 4
SUBS = 3
N = 16
ROWS = 80
CW = 512
QW = SUBS * CW
D = RINGS * QW
LEN = N * ROWS
F = 384
HEADS = F // HD
BQ = 256
BATCH = 4
SCALE2 = 1.4426950408889634 / (HD ** 0.5)


def ring_tp(ring, pos):
    a = lax.div(pos, 4)
    b = lax.rem(lax.rem(pos, 4) - a + 4, 4)
    return jnp.where(ring < 2, a * 4 + b, b * 4 + a)


def my_pos(ring, z, x):
    t = lax.rem(z + x, 4)
    return jnp.where(ring < 2, 4 * z + t, 4 * x + t)


def behind(ring, pos, k):
    up = lax.rem(ring, 2)
    return lax.rem(jnp.where(up == 0, pos + N - k, pos + k), N)


def main_kernel(
    len_ref, tok_ref, gain_ref, shift_ref, w_hbm, bq_ref, wo_hbm, bo_ref,
    out_ref, kv_hbm,
    ag, w, acc, qkv, att, wo, rs,
    ag_send, ag_recv, rs_send, rs_recv, w_sem, wo_sem, kv_sem,
):
    tp = lax.axis_index("tp")
    z = lax.div(tp, 4)
    x = lax.rem(tp, 4)
    pos = [my_pos(jnp.int32(r), z, x) for r in range(RINGS)]
    nxt = [ring_tp(jnp.int32(r), behind(jnp.int32(r), pos[r], N - 1)) for r in range(RINGS)]

    barrier = pltpu.get_barrier_semaphore()
    for r in range(RINGS):
        pl.semaphore_signal(barrier, inc=1, device_id={"tp": nxt[r]}, device_id_type=MESH)

    w_copies = [
        pltpu.make_async_copy(w_hbm.at[c], w.at[:, pl.ds(c * F, F)], w_sem.at[c]) for c in range(3)
    ]
    for copy in w_copies:
        copy.start()
    wo_copy = pltpu.make_async_copy(wo_hbm, wo, wo_sem)
    wo_copy.start()

    def norm_rows(i, carry):
        rows = pl.ds(pl.multiple_of(i * 16, 16), 16)
        v = tok_ref[rows, :].astype(jnp.float32)
        center = jnp.mean(v, axis=-1, keepdims=True)
        v = v - center
        spread = jnp.mean(v * v, axis=-1, keepdims=True)
        v = (v * lax.rsqrt(spread + EPS) * gain_ref[...] + shift_ref[...]).astype(jnp.bfloat16)
        for r in range(RINGS):
            for c in range(SUBS):
                ag[r, c, rows, :] = v[:, r * QW + c * CW : r * QW + (c + 1) * CW]
        return carry

    lax.fori_loop(0, ROWS // 16, norm_rows, 0)

    pl.semaphore_wait(barrier, RINGS)

    def slot(s):
        if isinstance(s, int):
            return pl.ds(s * ROWS, ROWS)
        return pl.ds(pl.multiple_of(s * ROWS, 16), ROWS)

    def ag_copy(r, c, s):
        return pltpu.make_async_remote_copy(
            src_ref=ag.at[r, c, slot(s)],
            dst_ref=ag.at[r, c, slot(s + 1)],
            send_sem=ag_send.at[r, c],
            recv_sem=ag_recv.at[r, c, s + 1],
            device_id={"tp": nxt[r]},
            device_id_type=MESH,
        )

    def ag_arrived(r, c, s):
        return pltpu.make_async_remote_copy(
            src_ref=ag.at[r, c, slot(s)],
            dst_ref=ag.at[r, c, slot(s)],
            send_sem=ag_send.at[r, c],
            recv_sem=ag_recv.at[r, c, s],
            device_id={"tp": nxt[r]},
            device_id_type=MESH,
        )

    for c in range(SUBS):
        for r in range(RINGS):
            ag_copy(r, c, 0).start()

    acc[...] = jnp.broadcast_to(bq_ref[...], acc.shape)
    for copy in w_copies:
        copy.wait()

    def unit(b, r, c):
        home = jnp.where(r < 2, 4 * z, 4 * x) + lax.rem(z + x, 4)
        a = ag[r, c, pl.ds(pl.multiple_of(b * (BATCH * ROWS), 64), BATCH * ROWS), :]
        wrow = pl.ds(pl.multiple_of(r * QW + c * CW, CW), CW)
        for lo, hi in ((0, 640), (640, 1152)):
            res = jnp.dot(a, w[wrow, lo:hi], preferred_element_type=jnp.float32)
            for i in range(BATCH):
                src = ring_tp(r, behind(r, home, b * BATCH + i))
                rows = pl.ds(pl.multiple_of(src * ROWS, 16), ROWS)
                acc[rows, lo:hi] += res[i * ROWS : (i + 1) * ROWS]

    def ag_step(s, carry):
        for c in range(SUBS):
            for r in range(RINGS):
                ag_arrived(r, c, s).wait_recv()
                ag_copy(r, c, s - 1).wait_send()
                ag_copy(r, c, s).start()

            @pl.when(s >= BATCH)
            def _():
                u = s - BATCH
                unit(lax.div(u, RINGS), lax.rem(u, RINGS), c)

        return carry

    lax.fori_loop(1, N - 1, ag_step, 0)
    for c in range(SUBS):
        for r in range(RINGS):
            ag_arrived(r, c, N - 1).wait_recv()
            ag_copy(r, c, N - 2).wait_send()

    def tail(u, carry):
        for c in range(SUBS):
            unit(lax.div(u, RINGS), lax.rem(u, RINGS), c)
        return carry

    lax.fori_loop(N - 1 - BATCH, N, tail, 0)

    def to_bf16(i, carry):
        rows = pl.ds(pl.multiple_of(i * 64, 64), 64)
        qkv[rows, :] = acc[rows, :].astype(jnp.bfloat16)
        return carry

    lax.fori_loop(0, LEN // 64, to_bf16, 0)
    kv_copy = pltpu.make_async_copy(qkv.at[:, pl.ds(F, 2 * F)], kv_hbm, kv_sem)
    kv_copy.start()

    last = len_ref[0] - 1

    def head(h, carry):
        col = pl.multiple_of(h * HD, HD)
        for qi in range(LEN // BQ):
            kv = (qi + 1) * BQ
            q = qkv[qi * BQ : (qi + 1) * BQ, pl.ds(col, HD)]
            k = qkv[0:kv, pl.ds(F + col, HD)]
            v = qkv[0:kv, pl.ds(2 * F + col, HD)]
            sc = lax.dot_general(q, k, (((1,), (1,)), ((), ())), preferred_element_type=jnp.float32)
            limit = jnp.minimum(lax.broadcasted_iota(jnp.int32, (BQ, 1), 0) + qi * BQ, last)
            sc = jnp.where(lax.broadcasted_iota(jnp.int32, (BQ, kv), 1) <= limit, sc, -1e30)
            top = jnp.max(sc, axis=-1, keepdims=True)
            e = jnp.exp2((sc - top) * SCALE2)
            inv = 1.0 / jnp.sum(e, axis=-1, keepdims=True)
            p = (e * inv).astype(jnp.bfloat16)
            o = jnp.dot(p, v, preferred_element_type=jnp.float32)
            att[qi * BQ : (qi + 1) * BQ, pl.ds(col, HD)] = o.astype(jnp.bfloat16)
        return carry

    lax.fori_loop(0, HEADS, head, 0)
    wo_copy.wait()

    def partial(r, c, s):
        src = ring_tp(jnp.int32(r), behind(jnp.int32(r), pos[r], s + 1))
        rows = pl.ds(pl.multiple_of(src * ROWS, 16), ROWS)
        lo = r * QW + c * CW
        return jnp.dot(att[rows, :], wo[:, lo : lo + CW], preferred_element_type=jnp.float32)

    def rs_copy(r, c, s):
        return pltpu.make_async_remote_copy(
            src_ref=rs.at[r, c, slot(s)],
            dst_ref=rs.at[r, c, slot(s + 1)],
            send_sem=rs_send.at[r, c],
            recv_sem=rs_recv.at[r, c, s + 1],
            device_id={"tp": nxt[r]},
            device_id_type=MESH,
        )

    def rs_arrived(r, c, s):
        return pltpu.make_async_remote_copy(
            src_ref=rs.at[r, c, slot(s)],
            dst_ref=rs.at[r, c, slot(s)],
            send_sem=rs_send.at[r, c],
            recv_sem=rs_recv.at[r, c, s],
            device_id={"tp": nxt[r]},
            device_id_type=MESH,
        )

    for c in range(SUBS):
        for r in range(RINGS):
            rs[r, c, slot(0), :] = partial(r, c, 0).astype(jnp.bfloat16)
            rs_copy(r, c, 0).start()

    def rs_step(s, carry):
        for c in range(SUBS):
            for r in range(RINGS):
                own = partial(r, c, s)
                rs_arrived(r, c, s).wait_recv()
                rs[r, c, slot(s), :] = (rs[r, c, slot(s), :].astype(jnp.float32) + own).astype(jnp.bfloat16)
                rs_copy(r, c, s - 1).wait_send()
                rs_copy(r, c, s).start()
        return carry

    lax.fori_loop(1, N - 1, rs_step, 0)
    for c in range(SUBS):
        for r in range(RINGS):
            lo = r * QW + c * CW
            own = partial(r, c, N - 1) + bo_ref[:, lo : lo + CW]
            rs_arrived(r, c, N - 1).wait_recv()
            rs_copy(r, c, N - 2).wait_send()
            out_ref[:, lo : lo + CW] = (rs[r, c, slot(N - 1), :].astype(jnp.float32) + own).astype(jnp.bfloat16)
    kv_copy.wait()


def cache_kernel(page_ref, len_ref, old_ref, new_ref, out_ref):
    page = page_ref[pl.program_id(0)]
    row = lax.broadcasted_iota(jnp.int32, (128, 1), 0) + page * 128
    written = (row < len_ref[0]) & (row >= 0)
    for i in range(2):
        out_ref[i, 0] = jnp.where(written, new_ref[:, i * F : (i + 1) * F], old_ref[i, 0])


def body(tokens, ln_gain, ln_bias, w_qkv, b_qkv, w_out, b_out, kv_cache, page_table, lengths):
    vmem = pl.BlockSpec(memory_space=pltpu.VMEM)
    anym = pl.BlockSpec(memory_space=pl.ANY)
    out, kv_new = pl.pallas_call(
        main_kernel,
        out_shape=(
            jax.ShapeDtypeStruct((ROWS, D), jnp.bfloat16),
            jax.ShapeDtypeStruct((LEN, 2 * F), jnp.bfloat16),
        ),
        in_specs=[pl.BlockSpec(memory_space=pltpu.SMEM), vmem, vmem, vmem, anym, vmem, anym, vmem],
        out_specs=(vmem, anym),
        scratch_shapes=[
            pltpu.VMEM((RINGS, SUBS, LEN, CW), jnp.bfloat16),
            pltpu.VMEM((D, 3 * F), jnp.bfloat16),
            pltpu.VMEM((LEN, 3 * F), jnp.float32),
            pltpu.VMEM((LEN, 3 * F), jnp.bfloat16),
            pltpu.VMEM((LEN, F), jnp.bfloat16),
            pltpu.VMEM((F, D), jnp.bfloat16),
            pltpu.VMEM((RINGS, SUBS, LEN, CW), jnp.bfloat16),
            pltpu.SemaphoreType.DMA((RINGS, SUBS)),
            pltpu.SemaphoreType.DMA((RINGS, SUBS, N)),
            pltpu.SemaphoreType.DMA((RINGS, SUBS)),
            pltpu.SemaphoreType.DMA((RINGS, SUBS, N)),
            pltpu.SemaphoreType.DMA((3,)),
            pltpu.SemaphoreType.DMA,
            pltpu.SemaphoreType.DMA,
        ],
        compiler_params=pltpu.CompilerParams(
            collective_id=0, has_side_effects=True, vmem_limit_bytes=67043328
        ),
        name="sublayer",
    )(
        lengths,
        tokens,
        ln_gain.reshape(1, D),
        ln_bias.reshape(1, D),
        jnp.transpose(w_qkv, (1, 0, 2)),
        b_qkv.reshape(1, 3 * F),
        w_out,
        b_out.reshape(1, D),
    )

    slots = kv_cache.shape[1]
    hit = page_table.reshape(1, -1) == jnp.arange(slots, dtype=jnp.int32)[:, None]
    pages = jnp.arange(page_table.size, dtype=jnp.int32)[None]
    page_of = jnp.max(jnp.where(hit, pages, -1), axis=1)
    kv_out = pl.pallas_call(
        cache_kernel,
        out_shape=jax.ShapeDtypeStruct(kv_cache.shape, kv_cache.dtype),
        grid_spec=pltpu.PrefetchScalarGridSpec(
            num_scalar_prefetch=2,
            grid=(slots,),
            in_specs=[
                pl.BlockSpec((2, 1, 128, F), lambda i, page, n: (0, i, 0, 0)),
                pl.BlockSpec((128, 2 * F), lambda i, page, n: (jnp.maximum(page[i], 0), 0)),
            ],
            out_specs=pl.BlockSpec((2, 1, 128, F), lambda i, page, n: (0, i, 0, 0)),
        ),
        name="cache_write",
    )(page_of, lengths, kv_cache, kv_new)
    return out, kv_out


def solution(mesh):
    placed = (
        P(("dp", "tp"), None),
        P(),
        P(),
        P(None, None, "tp"),
        P(None, "tp"),
        P("tp", None),
        P(),
        P(None, "dp", None, "tp"),
        P("dp", None),
        P("dp"),
    )
    return jax.shard_map(
        body,
        mesh=mesh,
        in_specs=placed,
        out_specs=(P(("dp", "tp"), None), P(None, "dp", None, "tp")),
        check_vma=False,
    )
```

```python
import functools

import jax
import jax.numpy as jnp
from jax import lax
from jax.experimental import pallas as pl
from jax.experimental.pallas import tpu as pltpu
from jax.sharding import PartitionSpec as P

HD = 128
EPS = 1e-05
MESH = pl.DeviceIdType.MESH
RINGS = 4
SUBS = 3
N = 16
ROWS = 80
CW = 512
QW = SUBS * CW
D = RINGS * QW
LEN = N * ROWS
F = 384
HEADS = F // HD
BQ = 320
BATCH = 4
PAGE = 128
PAGES = LEN // PAGE
SLOTS = 12
HC = D // 2
PR = F // 8
KX = 4 * F
CHUNKS = 12
LAG = 4
FORWARD_AT = 4
SCALE2 = 1.4426950408889634 / (HD ** 0.5)


def ring_tp(ring, pos):
    a = lax.div(pos, 4)
    b = lax.rem(lax.rem(pos, 4) - a + 4, 4)
    return jnp.where(ring < 2, a * 4 + b, b * 4 + a)


def my_pos(ring, z, x):
    t = lax.rem(z + x, 4)
    return jnp.where(ring < 2, 4 * z + t, 4 * x + t)


def behind(ring, pos, k):
    up = lax.rem(ring, 2)
    return lax.rem(jnp.where(up == 0, pos + N - k, pos + k), N)


def main_kernel(
    len_ref, page_ref, tok_ref, gain_ref, shift_ref, w_hbm, bq_ref, wo_hbm, bo_ref, old_hbm,
    out_ref, kv_hbm, g_hbm,
    ag, w, acc, qkv, att, wx, gat, psend, prec,
    ag_send, ag_recv, w_sem, kv_sem,
    g1_send, g1_recv, g2_send, g2_recv, gy_send, gy_recv, gf_send, gf_recv, gd_send, gd_recv,
    l_sem, at_send, at_recv, p_send, p_recv,
):
    tp = lax.axis_index("tp")
    dp = lax.axis_index("dp")
    z = lax.div(tp, 4)
    x = lax.rem(tp, 4)
    y = lax.div(dp, 2)
    core = lax.rem(dp, 2)
    pos = [my_pos(jnp.int32(r), z, x) for r in range(RINGS)]
    nxt = [ring_tp(jnp.int32(r), behind(jnp.int32(r), pos[r], N - 1)) for r in range(RINGS)]

    def along(axis, j):
        if axis == 0:
            return {"tp": z * 4 + lax.rem(x + j, 4)}
        return {"tp": lax.rem(z + j, 4) * 4 + x}

    def along_y(j):
        return {"dp": lax.rem(y + j, 4) * 2 + core}

    sibling = {"dp": y * 2 + 1 - core}

    barrier = pltpu.get_barrier_semaphore()
    peers = [along(a, j) for a in range(2) for j in (1, 2, 3)] + [along_y(1), along_y(3), sibling]
    for peer in peers:
        pl.semaphore_signal(barrier, inc=1, device_id=peer, device_id_type=MESH)

    w_copies = [
        pltpu.make_async_copy(w_hbm.at[c], w.at[:, pl.ds(c * F, F)], w_sem.at[c]) for c in range(3)
    ]
    for copy in w_copies:
        copy.start()
    pl.semaphore_wait(barrier, len(peers))

    def remote(src, dst, send_sem, recv_sem, device):
        return pltpu.make_async_remote_copy(
            src_ref=src, dst_ref=dst, send_sem=send_sem, recv_sem=recv_sem,
            device_id=device, device_id_type=MESH,
        )

    piece = pl.ds(pl.multiple_of((core * 4 + y) * PR, PR), PR)

    def g1_copy(axis, j):
        return remote(
            wo_hbm.at[piece, pl.ds(axis * HC, HC)], g_hbm.at[axis, 3 - j, piece],
            g1_send.at[axis, 3 - j], g1_recv.at[axis, 3 - j], along(axis, j),
        )

    def g2_copy(axis, j):
        k = 4 - j
        cols = pl.ds(0 if j == 1 else HC // 2, HC // 2)
        return remote(
            g_hbm.at[axis, k - 1, piece, cols], g_hbm.at[axis, 1, piece, cols],
            g2_send.at[axis, 3 - j], g2_recv.at[axis, 3 - j], along(axis, j),
        )

    for axis in range(2):
        for j in (1, 3):
            g1_copy(axis, j).start()

    def norm_rows(i, carry):
        rows = pl.ds(pl.multiple_of(i * 16, 16), 16)
        v = tok_ref[rows, :].astype(jnp.float32)
        center = jnp.mean(v, axis=-1, keepdims=True)
        v = v - center
        spread = jnp.mean(v * v, axis=-1, keepdims=True)
        v = (v * lax.rsqrt(spread + EPS) * gain_ref[...] + shift_ref[...]).astype(jnp.bfloat16)
        for r in range(RINGS):
            for c in range(SUBS):
                ag[r, c, rows, :] = v[:, r * QW + c * CW : r * QW + (c + 1) * CW]
        return carry

    lax.fori_loop(0, ROWS // 16, norm_rows, 0)

    def slot(s):
        if isinstance(s, int):
            return pl.ds(s * ROWS, ROWS)
        return pl.ds(pl.multiple_of(s * ROWS, 16), ROWS)

    def ag_copy(r, c, s):
        return remote(
            ag.at[r, c, slot(s)], ag.at[r, c, slot(s + 1)],
            ag_send.at[r, c], ag_recv.at[r, c, s + 1], {"tp": nxt[r]},
        )

    def ag_arrived(r, c, s):
        return remote(
            ag.at[r, c, slot(s)], ag.at[r, c, slot(s)],
            ag_send.at[r, c], ag_recv.at[r, c, s], {"tp": nxt[r]},
        )

    for r in range(RINGS):
        ag_copy(r, 0, 0).start()
    for j in (1, 3):
        for axis in range(2):
            g1_copy(axis, j).wait_recv()
            g2_copy(axis, j).start()
    for c in range(1, SUBS):
        for r in range(RINGS):
            ag_copy(r, c, 0).start()

    for c in range(3):
        acc[:, c * F : (c + 1) * F] = jnp.broadcast_to(bq_ref[c : c + 1, :], (LEN, F))
    for copy in w_copies:
        copy.wait()

    def gy_copy(axis, k, j):
        return remote(
            g_hbm.at[axis, k - 1, piece], g_hbm.at[axis, k - 1, piece],
            gy_send.at[axis, k - 1, j // 2], gy_recv.at[axis, k - 1, j // 2], along_y(j),
        )

    def gf_copy(axis, k):
        j = 1 if axis == 0 else 3
        src = pl.ds(pl.multiple_of((core * 4 + lax.rem(y + 4 - j, 4)) * PR, PR), PR)
        return remote(
            g_hbm.at[axis, k - 1, src], g_hbm.at[axis, k - 1, src],
            gf_send.at[axis, k - 1], gf_recv.at[axis, k - 1], along_y(j),
        )

    for k in (1, 3, 2):
        if k == 2:
            for axis in range(2):
                for j in (1, 3):
                    g2_copy(axis, j).wait_recv()
        for axis in range(2):
            gy_copy(axis, k, 1 if axis == 0 else 3).start()
    for k in (1, 3, 2):
        for axis in range(2):
            gy_copy(axis, k, 3 if axis == 0 else 1).start()

    def unit(b, r, c):
        home = jnp.where(r < 2, 4 * z, 4 * x) + lax.rem(z + x, 4)
        a = ag[r, c, pl.ds(pl.multiple_of(b * (BATCH * ROWS), 64), BATCH * ROWS), :]
        wrow = pl.ds(pl.multiple_of(r * QW + c * CW, CW), CW)
        for lo, hi in ((0, 640), (640, 1152)):
            res = jnp.dot(a, w[wrow, lo:hi], preferred_element_type=jnp.float32)
            for i in range(BATCH):
                src = ring_tp(r, behind(r, home, b * BATCH + i))
                rows = pl.ds(pl.multiple_of(src * ROWS, 16), ROWS)
                acc[rows, lo:hi] += res[i * ROWS : (i + 1) * ROWS]

    def ag_step(s, carry):
        for c in range(SUBS):
            for r in range(RINGS):
                ag_arrived(r, c, s).wait_recv()
                ag_copy(r, c, s - 1).wait_send()
                ag_copy(r, c, s).start()

            @pl.when(s >= BATCH)
            def _():
                u = s - BATCH
                unit(lax.div(u, RINGS), lax.rem(u, RINGS), c)

        for i, k in enumerate((1, 3, 2)):

            @pl.when(s == FORWARD_AT + i)
            def _():
                for axis in range(2):
                    gy_copy(axis, k, 1 if axis == 0 else 3).wait_recv()
                    gf_copy(axis, k).start()

        return carry

    lax.fori_loop(1, N - 1, ag_step, 0)
    for c in range(SUBS):
        for r in range(RINGS):
            ag_arrived(r, c, N - 1).wait_recv()
            ag_copy(r, c, N - 2).wait_send()

    mine = pl.ds(pl.multiple_of(core * (4 * PR), 4 * PR), 4 * PR)

    def gd_copy(axis, k):
        return remote(
            g_hbm.at[axis, k - 1, mine], g_hbm.at[axis, k - 1, mine],
            gd_send.at[axis, k - 1], gd_recv.at[axis, k - 1], sibling,
        )

    blocks = [(axis, k) for axis in range(2) for k in (1, 2, 3)]
    for axis, k in blocks:
        gy_copy(axis, k, 3 if axis == 0 else 1).wait_recv()
        gf_copy(axis, k).wait_recv()
        gd_copy(axis, k).start()

    def tail(u, carry):
        for c in range(SUBS):
            unit(lax.div(u, RINGS), lax.rem(u, RINGS), c)
        return carry

    lax.fori_loop(N - 1 - BATCH, N, tail, 0)

    def to_bf16(i, carry):
        rows = pl.ds(pl.multiple_of(i * 64, 64), 64)
        qkv[rows, :] = acc[rows, :].astype(jnp.bfloat16)
        return carry

    lax.fori_loop(0, LEN // 64, to_bf16, 0)

    half = SLOTS * PAGE // 2
    old_copies = [
        pltpu.make_async_copy(
            old_hbm.at[i, pl.ds(p * half, half)], ag.at[p, i, pl.ds(0, half), pl.ds(0, F)], kv_sem.at[p, i]
        )
        for p in range(2) for i in range(2)
    ]
    kv_copies = [
        pltpu.make_async_copy(
            ag.at[p, i, pl.ds(0, half), pl.ds(0, F)], kv_hbm.at[i, pl.ds(p * half, half)], kv_sem.at[p, i]
        )
        for p in range(2) for i in range(2)
    ]
    for copy in old_copies:
        copy.start()

    def home_of(n):
        if n < 8:
            return w, (n // 2) * KX, (n % 2) * CW
        return wx, 0, (n - 8) * CW

    def load(n, k):
        axis, m = n % 2, n // 2
        ref, row, col = home_of(n)
        if k == 0:
            src = wo_hbm.at[:, pl.ds(axis * HC + m * CW, CW)]
        else:
            src = g_hbm.at[axis, k - 1, :, pl.ds(m * CW, CW)]
        return pltpu.make_async_copy(src, ref.at[pl.ds(row + k * F, F), pl.ds(col, CW)], l_sem.at[n, k])

    for axis, k in blocks:
        gd_copy(axis, k).wait_recv()
    for n in range(CHUNKS):
        for k in range(4):
            load(n, k).start()

    last = len_ref[0] - 1

    def at_copy(axis, h, j):
        cols = pl.ds(pl.multiple_of(h * HD, HD), HD)
        there = pl.ds(pl.multiple_of((4 - j) * F + h * HD, HD), HD)
        if axis == 0:
            src = att.at[:, lax.rem(x + j, 4), :, cols]
        else:
            src = att.at[lax.rem(z + j, 4), :, :, cols]
        return remote(
            src, gat.at[axis, :, :, there], at_send.at[axis, h, j - 1], at_recv.at[axis, h, 3 - j],
            along(axis, j),
        )

    def head(h, carry):
        col = pl.multiple_of(h * HD, HD)
        for qi in range(LEN // BQ):
            kv = -(-(qi + 1) * BQ // HD) * HD
            q = qkv[qi * BQ : (qi + 1) * BQ, pl.ds(col, HD)]
            k = qkv[0:kv, pl.ds(F + col, HD)]
            v = qkv[0:kv, pl.ds(2 * F + col, HD)]
            sc = lax.dot_general(q, k, (((1,), (1,)), ((), ())), preferred_element_type=jnp.float32)
            limit = jnp.minimum(lax.broadcasted_iota(jnp.int32, (BQ, 1), 0) + qi * BQ, last)
            sc = jnp.where(lax.broadcasted_iota(jnp.int32, (BQ, kv), 1) <= limit, sc, -1e30)
            top = jnp.max(sc, axis=-1, keepdims=True)
            e = jnp.exp2((sc - top) * SCALE2)
            inv = 1.0 / jnp.sum(e, axis=-1, keepdims=True)
            p = (e * inv).astype(jnp.bfloat16)
            o = jnp.dot(p, v, preferred_element_type=jnp.float32)
            att[qi, :, :, pl.ds(col, HD)] = o.astype(jnp.bfloat16).reshape(4, ROWS, HD)
        for j in (2, 1, 3):
            for axis in range(2):
                at_copy(axis, h, j).start()
        return carry

    lax.fori_loop(0, HEADS, head, 0)
    for b in range(4):
        gat[0, b, :, 0:F] = att[b, x]
        gat[1, b, :, 0:F] = att[z, b]

    for copy in old_copies:
        copy.wait()

    def merge_slot(i, carry):
        plane, rows = lax.div(i, 6), pl.ds(pl.multiple_of(lax.rem(i, 6) * PAGE, PAGE), PAGE)
        row = lax.broadcasted_iota(jnp.int32, (PAGE, F), 0)
        for c in range(2):
            merged = ag[plane, c, rows, 0:F]
            for p in range(PAGES):
                here = (jnp.full((PAGE, F), page_ref[0, p], jnp.int32) == i) & (row + p * PAGE <= last)
                merged = jnp.where(here, qkv[p * PAGE : (p + 1) * PAGE, (1 + c) * F : (2 + c) * F], merged)
            ag[plane, c, rows, 0:F] = merged
        return carry

    lax.fori_loop(0, SLOTS, merge_slot, 0)
    for h in range(HEADS):
        for j in (1, 2, 3):
            for axis in range(2):
                at_copy(axis, h, j).wait_recv()
    for copy in kv_copies:
        copy.start()

    def p_copy(n, what):
        axis, ahead = 1 - n % 2, (1 if (n // 2) % 2 == 0 else 3)
        here = x if axis == 0 else z
        j = 4 - ahead if what == 2 else ahead
        block = lax.rem(here + (2 if what == 0 else j), 4)
        return remote(
            psend.at[n, block], prec.at[n, what], p_send.at[n, what], p_recv.at[n, what], along(axis, j)
        )

    def p_add(n):
        axis, ahead = 1 - n % 2, (1 if (n // 2) % 2 == 0 else 3)
        block = lax.rem((x if axis == 0 else z) + ahead, 4)
        p_copy(n, 0).wait_recv()
        both = psend[n, block].astype(jnp.float32) + prec[n, 0].astype(jnp.float32)
        psend[n, block] = both.astype(jnp.bfloat16)
        p_copy(n, 1).start()

    for n in range(CHUNKS):
        ref, row, col = home_of(n)
        for k in range(4):
            load(n, k).wait()
        a = gat[n % 2].reshape(4 * ROWS, KX)
        res = jnp.dot(a, ref[row : row + KX, col : col + CW], preferred_element_type=jnp.float32)
        psend[n] = res.astype(jnp.bfloat16).reshape(4, ROWS, CW)
        p_copy(n, 0).start()
        p_copy(n, 2).start()
        if n >= LAG:
            p_add(n - LAG)
    for n in range(CHUNKS - LAG, CHUNKS):
        p_add(n)

    for n in range(CHUNKS):
        here = z if n % 2 == 0 else x
        lo = (n % 2) * HC + (n // 2) * CW
        total = psend[n, here].astype(jnp.float32) + bo_ref[:, lo : lo + CW]
        p_copy(n, 2).wait_recv()
        total += prec[n, 2].astype(jnp.float32)
        p_copy(n, 1).wait_recv()
        total += prec[n, 1].astype(jnp.float32)
        out_ref[:, lo : lo + CW] = total.astype(jnp.bfloat16)

    for n in range(CHUNKS):
        for what in range(3):
            p_copy(n, what).wait_send()
    for axis in range(2):
        for j in (1, 3):
            g1_copy(axis, j).wait_send()
            g2_copy(axis, j).wait_send()
        for k in (1, 2, 3):
            gy_copy(axis, k, 1).wait_send()
            gy_copy(axis, k, 3).wait_send()
            gf_copy(axis, k).wait_send()
            gd_copy(axis, k).wait_send()
        for h in range(HEADS):
            for j in (1, 2, 3):
                at_copy(axis, h, j).wait_send()
    for copy in kv_copies:
        copy.wait()


def body(tokens, ln_gain, ln_bias, w_qkv, b_qkv, w_out, b_out, kv_cache, page_table, lengths):
    vmem = pl.BlockSpec(memory_space=pltpu.VMEM)
    anym = pl.BlockSpec(memory_space=pl.ANY)
    smem = pl.BlockSpec(memory_space=pltpu.SMEM)
    dma = pltpu.SemaphoreType.DMA
    out, kv_out, _ = pl.pallas_call(
        main_kernel,
        out_shape=(
            jax.ShapeDtypeStruct((ROWS, D), jnp.bfloat16),
            jax.ShapeDtypeStruct((2, SLOTS * PAGE, F), jnp.bfloat16),
            jax.ShapeDtypeStruct((2, 3, F, HC), jnp.bfloat16),
        ),
        in_specs=[smem, smem, vmem, vmem, vmem, anym, vmem, anym, vmem, anym],
        out_specs=(vmem, anym, anym),
        scratch_shapes=[
            pltpu.VMEM((RINGS, SUBS, LEN, CW), jnp.bfloat16),
            pltpu.VMEM((D, 3 * F), jnp.bfloat16),
            pltpu.VMEM((LEN, 3 * F), jnp.float32),
            pltpu.VMEM((LEN, 3 * F), jnp.bfloat16),
            pltpu.VMEM((4, 4, ROWS, F), jnp.bfloat16),
            pltpu.VMEM((KX, 4 * CW), jnp.bfloat16),
            pltpu.VMEM((2, 4, ROWS, KX), jnp.bfloat16),
            pltpu.VMEM((CHUNKS, 4, ROWS, CW), jnp.bfloat16),
            pltpu.VMEM((CHUNKS, 3, ROWS, CW), jnp.bfloat16),
            dma((RINGS, SUBS)),
            dma((RINGS, SUBS, N)),
            dma((3,)),
            dma((2, 2)),
            dma((2, 3)),
            dma((2, 3)),
            dma((2, 3)),
            dma((2, 3)),
            dma((2, 3, 2)),
            dma((2, 3, 2)),
            dma((2, 3)),
            dma((2, 3)),
            dma((2, 3)),
            dma((2, 3)),
            dma((CHUNKS, 4)),
            dma((2, HEADS, 3)),
            dma((2, HEADS, 3)),
            dma((CHUNKS, 3)),
            dma((CHUNKS, 3)),
        ],
        compiler_params=pltpu.CompilerParams(
            collective_id=0, has_side_effects=True, vmem_limit_bytes=67043328
        ),
        name="sublayer",
    )(
        lengths,
        page_table,
        tokens,
        ln_gain.reshape(1, D),
        ln_bias.reshape(1, D),
        jnp.transpose(w_qkv, (1, 0, 2)),
        b_qkv,
        w_out,
        b_out.reshape(1, D),
        kv_cache.reshape(2, SLOTS * PAGE, F),
    )
    return out, kv_out.reshape(kv_cache.shape)


def solution(mesh):
    placed = (
        P(("dp", "tp"), None),
        P(),
        P(),
        P(None, None, "tp"),
        P(None, "tp"),
        P("tp", None),
        P(),
        P(None, "dp", None, "tp"),
        P("dp", None),
        P("dp"),
    )
    return jax.shard_map(
        body,
        mesh=mesh,
        in_specs=placed,
        out_specs=(P(("dp", "tp"), None), P(None, "dp", None, "tp")),
        check_vma=False,
    )
```

```python
import functools

import jax
import jax.numpy as jnp
from jax import lax
from jax.experimental import pallas as pl
from jax.experimental.pallas import tpu as pltpu
from jax.sharding import PartitionSpec as P

HD = 128
EPS = 1e-05
MESH = pl.DeviceIdType.MESH
RINGS = 4
SUBS = 3
N = 16
ROWS = 80
CW = 512
QW = SUBS * CW
D = RINGS * QW
LEN = N * ROWS
F = 384
HEADS = F // HD
BQ = 320
BATCH = 4
PAGE = 128
PAGES = LEN // PAGE
SLOTS = 12
HC = D // 2
PR = F // 8
KX = 4 * F
CHUNKS = 12
LAG = 4
DIRECT = 8
FORWARD_AT = 4
SCALE2 = 1.4426950408889634 / (HD ** 0.5)


def ring_tp(ring, pos):
    a = lax.div(pos, 4)
    b = lax.rem(lax.rem(pos, 4) - a + 4, 4)
    return jnp.where(ring < 2, a * 4 + b, b * 4 + a)


def my_pos(ring, z, x):
    t = lax.rem(z + x, 4)
    return jnp.where(ring < 2, 4 * z + t, 4 * x + t)


def behind(ring, pos, k):
    up = lax.rem(ring, 2)
    return lax.rem(jnp.where(up == 0, pos + N - k, pos + k), N)


def main_kernel(
    len_ref, tok_ref, gain_ref, shift_ref, w_hbm, bq_ref, wo_hbm, bo_ref,
    out_ref, kv_hbm, g_hbm,
    ag, w, acc, qkv, att, wx, gat, psend, prec,
    ag_send, ag_recv, w_sem, kv_sem,
    g1_send, g1_recv, g2_send, g2_recv, gy_send, gy_recv, gf_send, gf_recv, gd_send, gd_recv,
    l_sem, at_send, at_recv, ax_send, ax_recv, p_send, p_recv,
):
    tp = lax.axis_index("tp")
    dp = lax.axis_index("dp")
    z = lax.div(tp, 4)
    x = lax.rem(tp, 4)
    y = lax.div(dp, 2)
    core = lax.rem(dp, 2)
    pos = [my_pos(jnp.int32(r), z, x) for r in range(RINGS)]
    nxt = [ring_tp(jnp.int32(r), behind(jnp.int32(r), pos[r], N - 1)) for r in range(RINGS)]

    def along(axis, j):
        if axis == 0:
            return {"tp": z * 4 + lax.rem(x + j, 4)}
        return {"tp": lax.rem(z + j, 4) * 4 + x}

    def along_y(j):
        return {"dp": lax.rem(y + j, 4) * 2 + core}

    sibling = {"dp": y * 2 + 1 - core}

    barrier = pltpu.get_barrier_semaphore()
    peers = [along(a, j) for a in range(2) for j in (1, 2, 3)] + [along_y(1), along_y(3), sibling]
    for peer in peers:
        pl.semaphore_signal(barrier, inc=1, device_id=peer, device_id_type=MESH)

    w_copies = [
        pltpu.make_async_copy(w_hbm.at[c], w.at[:, pl.ds(c * F, F)], w_sem.at[c]) for c in range(3)
    ]
    for copy in w_copies:
        copy.start()
    pl.semaphore_wait(barrier, len(peers))

    def remote(src, dst, send_sem, recv_sem, device):
        return pltpu.make_async_remote_copy(
            src_ref=src, dst_ref=dst, send_sem=send_sem, recv_sem=recv_sem,
            device_id=device, device_id_type=MESH,
        )

    piece = pl.ds(pl.multiple_of((core * 4 + y) * PR, PR), PR)

    def g1_copy(axis, j):
        return remote(
            wo_hbm.at[piece, pl.ds(axis * HC, HC)], g_hbm.at[axis, 3 - j, piece],
            g1_send.at[axis, 3 - j], g1_recv.at[axis, 3 - j], along(axis, j),
        )

    def g2_copy(axis, j):
        k = 4 - j
        cols = pl.ds(0 if j == 1 else HC // 2, HC // 2)
        return remote(
            g_hbm.at[axis, k - 1, piece, cols], g_hbm.at[axis, 1, piece, cols],
            g2_send.at[axis, 3 - j], g2_recv.at[axis, 3 - j], along(axis, j),
        )

    for axis in range(2):
        for j in (1, 3):
            g1_copy(axis, j).start()

    def norm_rows(i, carry):
        rows = pl.ds(pl.multiple_of(i * 16, 16), 16)
        v = tok_ref[rows, :].astype(jnp.float32)
        center = jnp.mean(v, axis=-1, keepdims=True)
        v = v - center
        spread = jnp.mean(v * v, axis=-1, keepdims=True)
        v = (v * lax.rsqrt(spread + EPS) * gain_ref[...] + shift_ref[...]).astype(jnp.bfloat16)
        for r in range(RINGS):
            for c in range(SUBS):
                ag[r, c, rows, :] = v[:, r * QW + c * CW : r * QW + (c + 1) * CW]
        return carry

    lax.fori_loop(0, ROWS // 16, norm_rows, 0)

    def slot(s):
        if isinstance(s, int):
            return pl.ds(s * ROWS, ROWS)
        return pl.ds(pl.multiple_of(s * ROWS, 16), ROWS)

    def ag_copy(r, c, s):
        return remote(
            ag.at[r, c, slot(s)], ag.at[r, c, slot(s + 1)],
            ag_send.at[r, c], ag_recv.at[r, c, s + 1], {"tp": nxt[r]},
        )

    def ag_arrived(r, c, s):
        return remote(
            ag.at[r, c, slot(s)], ag.at[r, c, slot(s)],
            ag_send.at[r, c], ag_recv.at[r, c, s], {"tp": nxt[r]},
        )

    for r in range(RINGS):
        ag_copy(r, 0, 0).start()
    for j in (1, 3):
        for axis in range(2):
            g1_copy(axis, j).wait_recv()
            g2_copy(axis, j).start()
    for c in range(1, SUBS):
        for r in range(RINGS):
            ag_copy(r, c, 0).start()

    for c in range(3):
        acc[:, c * F : (c + 1) * F] = jnp.broadcast_to(bq_ref[c : c + 1, :], (LEN, F))
    for copy in w_copies:
        copy.wait()

    def gy_copy(axis, k, j):
        return remote(
            g_hbm.at[axis, k - 1, piece], g_hbm.at[axis, k - 1, piece],
            gy_send.at[axis, k - 1, j // 2], gy_recv.at[axis, k - 1, j // 2], along_y(j),
        )

    def gf_copy(axis, k):
        j = 1 if axis == 0 else 3
        src = pl.ds(pl.multiple_of((core * 4 + lax.rem(y + 4 - j, 4)) * PR, PR), PR)
        return remote(
            g_hbm.at[axis, k - 1, src], g_hbm.at[axis, k - 1, src],
            gf_send.at[axis, k - 1], gf_recv.at[axis, k - 1], along_y(j),
        )

    for k in (1, 3, 2):
        if k == 2:
            for axis in range(2):
                for j in (1, 3):
                    g2_copy(axis, j).wait_recv()
        for axis in range(2):
            gy_copy(axis, k, 1 if axis == 0 else 3).start()
    for k in (1, 3, 2):
        for axis in range(2):
            gy_copy(axis, k, 3 if axis == 0 else 1).start()

    def unit(first, count, r, subs, cols):
        home = jnp.where(r < 2, 4 * z, 4 * x) + lax.rem(z + x, 4)
        rows = pl.ds(pl.multiple_of(first * ROWS, 16), count * ROWS)
        for lo, hi in cols:
            res = None
            for c in subs:
                wrow = pl.ds(pl.multiple_of(r * QW + c * CW, CW), CW)
                part = jnp.dot(ag[r, c, rows, :], w[wrow, lo:hi], preferred_element_type=jnp.float32)
                res = part if res is None else res + part
            for i in range(count):
                src = ring_tp(r, behind(r, home, first + i))
                to = pl.ds(pl.multiple_of(src * ROWS, 16), ROWS)
                acc[to, lo:hi] += res[i * ROWS : (i + 1) * ROWS]

    halves, whole = ((0, 640), (640, 1152)), ((0, 1152),)

    mine = pl.ds(pl.multiple_of(core * (4 * PR), 4 * PR), 4 * PR)

    def gd_copy(axis, k):
        return remote(
            g_hbm.at[axis, k - 1, mine], g_hbm.at[axis, k - 1, mine],
            gd_send.at[axis, k - 1], gd_recv.at[axis, k - 1], sibling,
        )

    blocks = [(axis, k) for axis in range(2) for k in (1, 2, 3)]

    def ag_step(s, carry):
        first = jnp.where(s < 12, s - 4, 2 * s - 16)
        count = jnp.where(s < 4, 0, jnp.where(s < 12, 1, jnp.where(s < 14, 2, 0)))
        for c in range(SUBS):
            for r in range(RINGS):
                ag_arrived(r, c, s).wait_recv()
                ag_copy(r, c, s - 1).wait_send()
                ag_copy(r, c, s).start()

            def four(u, carry, c=c):
                unit(lax.div(u, RINGS) * 4, 4, lax.rem(u, RINGS), (c,), halves)
                return carry

            lax.fori_loop(first, first + count, four, 0)

        for i, k in enumerate((1, 3, 2)):

            @pl.when(s == FORWARD_AT + i)
            def _():
                for axis in range(2):
                    gy_copy(axis, k, 1 if axis == 0 else 3).wait_recv()
                    gf_copy(axis, k).start()

        @pl.when(s == 13)
        def _():
            for axis, k in blocks:
                gy_copy(axis, k, 3 if axis == 0 else 1).wait_recv()
                gf_copy(axis, k).wait_recv()
                gd_copy(axis, k).start()

        return carry

    lax.fori_loop(1, N - 1, ag_step, 0)

    def two(first):
        def step(r, carry):
            unit(first, 2, r, (0, 1, 2), whole)
            return carry

        lax.fori_loop(0, RINGS, step, 0)

    two(12)
    for c in range(SUBS):
        for r in range(RINGS):
            ag_arrived(r, c, N - 1).wait_recv()
            ag_copy(r, c, N - 2).wait_send()
    two(14)

    def to_bf16(i, carry):
        rows = pl.ds(pl.multiple_of(i * 64, 64), 64)
        qkv[rows, :] = acc[rows, :].astype(jnp.bfloat16)
        return carry

    lax.fori_loop(0, LEN // 64, to_bf16, 0)

    kv_copy = pltpu.make_async_copy(qkv.at[:, pl.ds(F, 2 * F)], kv_hbm, kv_sem)
    kv_copy.start()

    def home_of(n):
        if n < 8:
            return w, (n // 2) * KX, (n % 2) * CW
        return wx, 0, (n - 8) * CW

    def load(n, k):
        axis, m = n % 2, n // 2
        ref, row, col = home_of(n)
        if k == 0:
            src = wo_hbm.at[:, pl.ds(axis * HC + m * CW, CW)]
        else:
            src = g_hbm.at[axis, k - 1, :, pl.ds(m * CW, CW)]
        return pltpu.make_async_copy(src, ref.at[pl.ds(row + k * F, F), pl.ds(col, CW)], l_sem.at[n, k])

    for axis, k in blocks:
        gd_copy(axis, k).wait_recv()
    for n in range(CHUNKS):
        for k in range(4):
            load(n, k).start()

    last = len_ref[0] - 1

    def az_copy(h, qi, k):
        src = att.at[qi, :, :, pl.ds(pl.multiple_of(h * HD, HD), HD)]
        there = pl.ds(pl.multiple_of(k * F + h * HD, HD), HD)
        return remote(
            src, gat.at[1, :, :, there], at_send.at[h, k - 1], at_recv.at[h, k - 1], {"tp": qi * 4 + x}
        )

    def ax_copy(h, qi, j):
        src = att.at[qi, lax.rem(x + j, 4), :, pl.ds(pl.multiple_of(h * HD, HD), HD)]
        there = pl.ds(pl.multiple_of((4 - j) * F + h * HD, HD), HD)
        return remote(
            src, gat.at[0, qi, :, there], ax_send.at[h, qi, j - 1], ax_recv.at[h, qi, 3 - j], along(0, j)
        )

    def head(h, carry):
        col = pl.multiple_of(h * HD, HD)
        for qi in range(LEN // BQ):
            kv = -(-(qi + 1) * BQ // HD) * HD
            free = min(qi * BQ // HD * HD, LEN // 2)
            q = qkv[qi * BQ : (qi + 1) * BQ, pl.ds(col, HD)]
            limit = jnp.minimum(lax.broadcasted_iota(jnp.int32, (BQ, 1), 0) + qi * BQ, last)
            parts = []
            for lo, hi in ((0, free), (free, kv)):
                if hi > lo:
                    k = qkv[lo:hi, pl.ds(F + col, HD)]
                    sc = lax.dot_general(q, k, (((1,), (1,)), ((), ())), preferred_element_type=jnp.float32)
                    if lo == free:
                        sc = jnp.where(lax.broadcasted_iota(jnp.int32, (BQ, hi - lo), 1) + lo <= limit, sc, -1e30)
                    parts.append((lo, hi, sc))
            top = functools.reduce(jnp.maximum, [jnp.max(sc, axis=-1, keepdims=True) for _, _, sc in parts])
            parts = [(lo, hi, jnp.exp2((sc - top) * SCALE2)) for lo, hi, sc in parts]
            inv = 1.0 / sum(jnp.sum(e, axis=-1, keepdims=True) for _, _, e in parts)
            o = sum(
                jnp.dot(
                    (e * inv).astype(jnp.bfloat16),
                    qkv[lo:hi, pl.ds(2 * F + col, HD)],
                    preferred_element_type=jnp.float32,
                )
                for lo, hi, e in parts
            )
            att[qi, :, :, pl.ds(col, HD)] = o.astype(jnp.bfloat16).reshape(4, ROWS, HD)
            for j in (2, 1, 3):
                ax_copy(h, qi, j).start()

            @pl.when(z != qi)
            def _():
                az_copy(h, qi, lax.rem(z - qi + 4, 4)).start()

        return carry

    lax.fori_loop(0, HEADS, head, 0)
    for b in range(4):
        gat[0, b, :, 0:F] = att[b, x]
        gat[1, b, :, 0:F] = att[z, b]

    for h in range(HEADS):
        for k in (1, 2, 3):
            az_copy(h, 0, k).wait_recv()
            for qi in range(LEN // BQ):
                ax_copy(h, qi, k).wait_recv()

    def p_copy(n, what):
        axis, ahead = 1 - n % 2, (1 if (n // 2) % 2 == 0 else 3)
        here = x if axis == 0 else z
        j = (2 if n >= DIRECT else ahead, ahead, 4 - ahead)[what]
        block = lax.rem(here + (2 if what == 0 else j), 4)
        return remote(
            psend.at[n, block], prec.at[n, what], p_send.at[n, what], p_recv.at[n, what], along(axis, j)
        )

    def p_add(n):
        axis, ahead = 1 - n % 2, (1 if (n // 2) % 2 == 0 else 3)
        block = lax.rem((x if axis == 0 else z) + ahead, 4)
        p_copy(n, 0).wait_recv()
        both = psend[n, block].astype(jnp.float32) + prec[n, 0].astype(jnp.float32)
        psend[n, block] = both.astype(jnp.bfloat16)
        p_copy(n, 1).start()

    for n in range(CHUNKS):
        ref, row, col = home_of(n)
        for k in range(4):
            load(n, k).wait()
        a = gat[n % 2].reshape(4 * ROWS, KX)
        res = jnp.dot(a, ref[row : row + KX, col : col + CW], preferred_element_type=jnp.float32)
        psend[n] = res.astype(jnp.bfloat16).reshape(4, ROWS, CW)
        for what in range(3):
            if n >= DIRECT or what != 1:
                p_copy(n, what).start()
        if 0 <= n - LAG < DIRECT:
            p_add(n - LAG)
    for n in range(CHUNKS - LAG, DIRECT):
        p_add(n)

    for n in range(CHUNKS):
        here = z if n % 2 == 0 else x
        lo = (n % 2) * HC + (n // 2) * CW
        total = psend[n, here].astype(jnp.float32) + bo_ref[:, lo : lo + CW]
        p_copy(n, 2).wait_recv()
        total += prec[n, 2].astype(jnp.float32)
        p_copy(n, 1).wait_recv()
        total += prec[n, 1].astype(jnp.float32)
        if n >= DIRECT:
            p_copy(n, 0).wait_recv()
            total += prec[n, 0].astype(jnp.float32)
        out_ref[:, lo : lo + CW] = total.astype(jnp.bfloat16)

    for n in range(CHUNKS):
        for what in range(3):
            p_copy(n, what).wait_send()
    for axis in range(2):
        for j in (1, 3):
            g1_copy(axis, j).wait_send()
            g2_copy(axis, j).wait_send()
        for k in (1, 2, 3):
            gy_copy(axis, k, 1).wait_send()
            gy_copy(axis, k, 3).wait_send()
            gf_copy(axis, k).wait_send()
            gd_copy(axis, k).wait_send()
    for h in range(HEADS):
        for k in (1, 2, 3):
            az_copy(h, 0, k).wait_send()
            for qi in range(LEN // BQ):
                ax_copy(h, qi, k).wait_send()
    kv_copy.wait()


def finish_kernel(page_ref, len_ref, part_hbm, new_hbm, old_hbm, out_hbm, kv_hbm, part, new, kv, in_sem, out_sem):
    group = SLOTS * PAGE // 4
    news = [
        pltpu.make_async_copy(new_hbm.at[pl.ds(g * BQ, BQ)], new.at[pl.ds(g * BQ, BQ)], in_sem.at[g])
        for g in range(4)
    ]
    olds = [
        pltpu.make_async_copy(
            old_hbm.at[:, pl.ds(g * group, group)], kv.at[:, pl.ds(g * group, group)], in_sem.at[4 + g]
        )
        for g in range(4)
    ]
    kvs = [
        pltpu.make_async_copy(
            kv.at[:, pl.ds(g * group, group)], kv_hbm.at[:, pl.ds(g * group, group)], out_sem.at[g]
        )
        for g in range(4)
    ]
    load = pltpu.make_async_copy(part_hbm, part, in_sem.at[8])
    store = pltpu.make_async_copy(part, out_hbm, out_sem.at[4])
    for copy in [*news, *olds, load]:
        copy.start()
    for copy in news:
        copy.wait()
    for g in range(4):
        olds[g].wait()
        for i in range(g * SLOTS // 4, (g + 1) * SLOTS // 4):
            page = jnp.int32(-1)
            for p in range(PAGES):
                page = jnp.where(page_ref[0, p] == i, p, page)
            row = lax.broadcasted_iota(jnp.int32, (PAGE, 1), 0) + page * PAGE
            written = (row < len_ref[0]) & (row >= 0)
            rows = pl.ds(pl.multiple_of(jnp.maximum(page, 0) * PAGE, PAGE), PAGE)
            for c in range(2):
                old = kv[c, i * PAGE : (i + 1) * PAGE, :]
                kv[c, i * PAGE : (i + 1) * PAGE, :] = jnp.where(written, new[rows, c * F : (c + 1) * F], old)
        kvs[g].start()
    load.wait()
    store.start()
    for copy in [*kvs, store]:
        copy.wait()


def body(tokens, ln_gain, ln_bias, w_qkv, b_qkv, w_out, b_out, kv_cache, page_table, lengths):
    vmem = pl.BlockSpec(memory_space=pltpu.VMEM)
    anym = pl.BlockSpec(memory_space=pl.ANY)
    smem = pl.BlockSpec(memory_space=pltpu.SMEM)
    dma = pltpu.SemaphoreType.DMA
    part, kv_new, _ = pl.pallas_call(
        main_kernel,
        out_shape=(
            jax.ShapeDtypeStruct((ROWS, D), jnp.bfloat16),
            jax.ShapeDtypeStruct((LEN, 2 * F), jnp.bfloat16),
            jax.ShapeDtypeStruct((2, 3, F, HC), jnp.bfloat16),
        ),
        in_specs=[smem, vmem, vmem, vmem, anym, vmem, anym, vmem],
        out_specs=(vmem, anym, anym),
        scratch_shapes=[
            pltpu.VMEM((RINGS, SUBS, LEN, CW), jnp.bfloat16),
            pltpu.VMEM((D, 3 * F), jnp.bfloat16),
            pltpu.VMEM((LEN, 3 * F), jnp.float32),
            pltpu.VMEM((LEN, 3 * F), jnp.bfloat16),
            pltpu.VMEM((4, 4, ROWS, F), jnp.bfloat16),
            pltpu.VMEM((KX, 4 * CW), jnp.bfloat16),
            pltpu.VMEM((2, 4, ROWS, KX), jnp.bfloat16),
            pltpu.VMEM((CHUNKS, 4, ROWS, CW), jnp.bfloat16),
            pltpu.VMEM((CHUNKS, 3, ROWS, CW), jnp.bfloat16),
            dma((RINGS, SUBS)),
            dma((RINGS, SUBS, N)),
            dma((3,)),
            dma,
            dma((2, 3)),
            dma((2, 3)),
            dma((2, 3)),
            dma((2, 3)),
            dma((2, 3, 2)),
            dma((2, 3, 2)),
            dma((2, 3)),
            dma((2, 3)),
            dma((2, 3)),
            dma((2, 3)),
            dma((CHUNKS, 4)),
            dma((HEADS, 3)),
            dma((HEADS, 3)),
            dma((HEADS, 4, 3)),
            dma((HEADS, 4, 3)),
            dma((CHUNKS, 3)),
            dma((CHUNKS, 3)),
        ],
        compiler_params=pltpu.CompilerParams(
            collective_id=0, has_side_effects=True, vmem_limit_bytes=67043328
        ),
        name="sublayer",
    )(
        lengths,
        tokens,
        ln_gain.reshape(1, D),
        ln_bias.reshape(1, D),
        jnp.transpose(w_qkv, (1, 0, 2)),
        b_qkv,
        w_out,
        b_out.reshape(1, D),
    )
    out, kv_out = pl.pallas_call(
        finish_kernel,
        out_shape=(
            jax.ShapeDtypeStruct((ROWS, D), jnp.bfloat16),
            jax.ShapeDtypeStruct((2, SLOTS * PAGE, F), jnp.bfloat16),
        ),
        in_specs=[smem, smem, anym, anym, anym],
        out_specs=(anym, anym),
        scratch_shapes=[
            pltpu.VMEM((ROWS, D), jnp.bfloat16),
            pltpu.VMEM((LEN, 2 * F), jnp.bfloat16),
            pltpu.VMEM((2, SLOTS * PAGE, F), jnp.bfloat16),
            dma((9,)),
            dma((5,)),
        ],
        name="finish",
    )(page_table, lengths, part, kv_new, kv_cache.reshape(2, SLOTS * PAGE, F))
    return out, kv_out.reshape(kv_cache.shape)


def solution(mesh):
    placed = (
        P(("dp", "tp"), None),
        P(),
        P(),
        P(None, None, "tp"),
        P(None, "tp"),
        P("tp", None),
        P(),
        P(None, "dp", None, "tp"),
        P("dp", None),
        P("dp"),
    )
    return jax.shard_map(
        body,
        mesh=mesh,
        in_specs=placed,
        out_specs=(P(("dp", "tp"), None), P(None, "dp", None, "tp")),
        check_vma=False,
    )
```

```python
import functools

import jax
import jax.numpy as jnp
from jax import lax
from jax.experimental import pallas as pl
from jax.experimental.pallas import tpu as pltpu
from jax.sharding import PartitionSpec as P

HD = 128
EPS = 1e-05
MESH = pl.DeviceIdType.MESH
RINGS = 4
SUBS = 3
N = 16
ROWS = 80
CW = 512
QW = SUBS * CW
D = RINGS * QW
LEN = N * ROWS
F = 384
HEADS = F // HD
BQ = 320
BATCH = 4
PAGE = 128
PAGES = LEN // PAGE
SLOTS = 12
HC = D // 2
PR = F // 8
KX = 4 * F
CHUNKS = 12
LAG = 4
RC = 160
SPAN = 4
FORWARD_AT = 4
SCALE2 = 1.4426950408889634 / (HD ** 0.5)


def ring_tp(ring, pos):
    a = lax.div(pos, 4)
    b = lax.rem(lax.rem(pos, 4) - a + 4, 4)
    return jnp.where(ring < 2, a * 4 + b, b * 4 + a)


def my_pos(ring, z, x):
    t = lax.rem(z + x, 4)
    return jnp.where(ring < 2, 4 * z + t, 4 * x + t)


def behind(ring, pos, k):
    up = lax.rem(ring, 2)
    return lax.rem(jnp.where(up == 0, pos + N - k, pos + k), N)


def main_kernel(
    len_ref, tok_ref, gain_ref, shift_ref, w_hbm, bq_ref, wo_hbm, bo_ref,
    out_ref, kv_hbm, g_hbm,
    ag, w, acc, qkv, att, wx, gat, psend, prec, sbuf, out,
    ag_send, ag_recv, w_sem, kv_sem, out_sem,
    g_send, g1_recv, g2_recv, gy_recv, gf_recv, gd_recv,
    l_sem, az_send, az_recv, ax_send, ax_recv, p_send, p0_recv, p_recv,
):
    tp = lax.axis_index("tp")
    dp = lax.axis_index("dp")
    z = lax.div(tp, 4)
    x = lax.rem(tp, 4)
    y = lax.div(dp, 2)
    core = lax.rem(dp, 2)
    pos = [my_pos(jnp.int32(r), z, x) for r in range(RINGS)]
    nxt = [ring_tp(jnp.int32(r), behind(jnp.int32(r), pos[r], N - 1)) for r in range(RINGS)]

    def along(axis, j):
        if axis == 0:
            return {"tp": z * 4 + lax.rem(x + j, 4)}
        return {"tp": lax.rem(z + j, 4) * 4 + x}

    def along_y(j):
        return {"dp": lax.rem(y + j, 4) * 2 + core}

    sibling = {"dp": y * 2 + 1 - core}

    barrier = pltpu.get_barrier_semaphore()
    peers = [along(a, j) for a in range(2) for j in (1, 2, 3)] + [along_y(1), along_y(3), sibling]
    for peer in peers:
        pl.semaphore_signal(barrier, inc=1, device_id=peer, device_id_type=MESH)

    w_copies = [
        pltpu.make_async_copy(w_hbm.at[c], w.at[:, pl.ds(c * F, F)], w_sem) for c in range(3)
    ]
    for copy in w_copies:
        copy.start()
    pl.semaphore_wait(barrier, len(peers))

    def remote(src, dst, send_sem, recv_sem, device):
        return pltpu.make_async_remote_copy(
            src_ref=src, dst_ref=dst, send_sem=send_sem, recv_sem=recv_sem,
            device_id=device, device_id_type=MESH,
        )

    piece = pl.ds(pl.multiple_of((core * 4 + y) * PR, PR), PR)

    def g1_copy(axis, j):
        return remote(
            wo_hbm.at[piece, pl.ds(axis * HC, HC)], g_hbm.at[axis, 3 - j, piece],
            g_send.at[0], g1_recv.at[axis, j // 2], along(axis, j),
        )

    def g2_copy(axis, j):
        k = 4 - j
        cols = pl.ds(0 if j == 1 else HC // 2, HC // 2)
        return remote(
            g_hbm.at[axis, k - 1, piece, cols], g_hbm.at[axis, 1, piece, cols],
            g_send.at[1], g2_recv.at[axis, j // 2], along(axis, j),
        )

    for axis in range(2):
        for j in (1, 3):
            g1_copy(axis, j).start()

    def norm_rows(i, carry):
        rows = pl.ds(pl.multiple_of(i * 16, 16), 16)
        v = tok_ref[rows, :].astype(jnp.float32)
        center = jnp.mean(v, axis=-1, keepdims=True)
        v = v - center
        spread = jnp.mean(v * v, axis=-1, keepdims=True)
        v = (v * lax.rsqrt(spread + EPS) * gain_ref[...] + shift_ref[...]).astype(jnp.bfloat16)
        for r in range(RINGS):
            for c in range(SUBS):
                ag[r, c, rows, :] = v[:, r * QW + c * CW : r * QW + (c + 1) * CW]
        return carry

    lax.fori_loop(0, ROWS // 16, norm_rows, 0)

    def slot(s):
        if isinstance(s, int):
            return pl.ds(s * ROWS, ROWS)
        return pl.ds(pl.multiple_of(s * ROWS, 16), ROWS)

    def ag_copy(r, c, s):
        return remote(
            ag.at[r, c, slot(s)], ag.at[r, c, slot(s + 1)],
            ag_send.at[r, c], ag_recv.at[r, c, lax.rem(s + 1, SPAN)], {"tp": nxt[r]},
        )

    def ag_arrived(r, c, s):
        return remote(
            ag.at[r, c, slot(s)], ag.at[r, c, slot(s)],
            ag_send.at[r, c], ag_recv.at[r, c, lax.rem(s, SPAN)], {"tp": nxt[r]},
        )

    for r in range(RINGS):
        ag_copy(r, 0, 0).start()
    for j in (1, 3):
        for axis in range(2):
            g1_copy(axis, j).wait_recv()
            g2_copy(axis, j).start()
    for c in range(1, SUBS):
        for r in range(RINGS):
            ag_copy(r, c, 0).start()

    for c in range(3):
        acc[:, c * F : (c + 1) * F] = jnp.broadcast_to(bq_ref[c : c + 1, :], (LEN, F))
    pltpu.make_async_copy(w, w, w_sem).wait()

    def gy_copy(axis, k, j):
        return remote(
            g_hbm.at[axis, k - 1, piece], g_hbm.at[axis, k - 1, piece],
            g_send.at[2 + axis], gy_recv.at[axis, k - 1, j // 2], along_y(j),
        )

    def gf_copy(axis, k):
        j = 1 if axis == 0 else 3
        src = pl.ds(pl.multiple_of((core * 4 + lax.rem(y + 4 - j, 4)) * PR, PR), PR)
        return remote(
            g_hbm.at[axis, k - 1, src], g_hbm.at[axis, k - 1, src],
            g_send.at[4], gf_recv.at[axis, k - 1], along_y(j),
        )

    for k in (1, 3, 2):
        if k == 2:
            for axis in range(2):
                for j in (1, 3):
                    g2_copy(axis, j).wait_recv()
        for axis in range(2):
            gy_copy(axis, k, 1 if axis == 0 else 3).start()
    for k in (1, 3, 2):
        for axis in range(2):
            gy_copy(axis, k, 3 if axis == 0 else 1).start()

    def unit(first, count, r, subs, cols):
        home = jnp.where(r < 2, 4 * z, 4 * x) + lax.rem(z + x, 4)
        rows = pl.ds(pl.multiple_of(first * ROWS, 16), count * ROWS)
        for lo, hi in cols:
            res = None
            for c in subs:
                wrow = pl.ds(pl.multiple_of(r * QW + c * CW, CW), CW)
                part = jnp.dot(ag[r, c, rows, :], w[wrow, lo:hi], preferred_element_type=jnp.float32)
                res = part if res is None else res + part
            for i in range(count):
                src = ring_tp(r, behind(r, home, first + i))
                to = pl.ds(pl.multiple_of(src * ROWS, 16), ROWS)
                acc[to, lo:hi] += res[i * ROWS : (i + 1) * ROWS]

    halves, whole = ((0, 640), (640, 1152)), ((0, 1152),)

    mine = pl.ds(pl.multiple_of(core * (4 * PR), 4 * PR), 4 * PR)

    def gd_copy(axis, k):
        return remote(
            g_hbm.at[axis, k - 1, mine], g_hbm.at[axis, k - 1, mine],
            g_send.at[5], gd_recv.at[axis, k - 1], sibling,
        )

    blocks = [(axis, k) for axis in range(2) for k in (1, 2, 3)]

    def ag_step(s, carry):
        first = jnp.where(s < 12, s - 4, 2 * s - 16)
        count = jnp.where(s < 4, 0, jnp.where(s < 12, 1, jnp.where(s < 14, 2, 0)))
        for c in range(SUBS):
            for r in range(RINGS):
                ag_arrived(r, c, s).wait_recv()
                ag_copy(r, c, s - 1).wait_send()
                ag_copy(r, c, s).start()

            def four(u, carry, c=c):
                unit(lax.div(u, RINGS) * 4, 4, lax.rem(u, RINGS), (c,), halves)
                return carry

            lax.fori_loop(first, first + count, four, 0)

        for i, k in enumerate((1, 3, 2)):

            @pl.when(s == FORWARD_AT + i)
            def _():
                for axis in range(2):
                    gy_copy(axis, k, 1 if axis == 0 else 3).wait_recv()
                    gf_copy(axis, k).start()

        @pl.when(s == 13)
        def _():
            for axis, k in blocks:
                gy_copy(axis, k, 3 if axis == 0 else 1).wait_recv()
                gf_copy(axis, k).wait_recv()
                gd_copy(axis, k).start()

        return carry

    lax.fori_loop(1, N - 1, ag_step, 0)

    def two(first):
        def step(r, carry):
            unit(first, 2, r, (0, 1, 2), whole)
            return carry

        lax.fori_loop(0, RINGS, step, 0)

    two(12)
    for c in range(SUBS):
        for r in range(RINGS):
            ag_arrived(r, c, N - 1).wait_recv()
            ag_copy(r, c, N - 2).wait_send()
    two(14)

    def to_bf16(i, carry):
        rows = pl.ds(pl.multiple_of(i * 64, 64), 64)
        qkv[rows, :] = acc[rows, :].astype(jnp.bfloat16)
        return carry

    lax.fori_loop(0, LEN // 64, to_bf16, 0)

    kv_copy = pltpu.make_async_copy(qkv.at[:, pl.ds(F, 2 * F)], kv_hbm, kv_sem)
    kv_copy.start()

    def home_of(n):
        if n < 8:
            return w, (n // 2) * KX, (n % 2) * CW
        return wx, 0, (n - 8) * CW

    def load(n, k):
        axis, m = n % 2, n // 2
        ref, row, col = home_of(n)
        if k == 0:
            src = wo_hbm.at[:, pl.ds(axis * HC + m * CW, CW)]
        else:
            src = g_hbm.at[axis, k - 1, :, pl.ds(m * CW, CW)]
        return pltpu.make_async_copy(src, ref.at[pl.ds(row + k * F, F), pl.ds(col, CW)], l_sem.at[n])

    def loaded(n):
        ref, row, col = home_of(n)
        chunk = ref.at[pl.ds(row, KX), pl.ds(col, CW)]
        return pltpu.make_async_copy(chunk, chunk, l_sem.at[n])

    last = len_ref[0] - 1

    def az_copy(h, qi, k):
        src = att.at[qi, :, :, pl.ds(pl.multiple_of(h * HD, HD), HD)]
        there = pl.ds(pl.multiple_of(k * F + h * HD, HD), HD)
        return remote(
            src, gat.at[1, :, :, there], az_send.at[h, k - 1], az_recv.at[h, k - 1], {"tp": qi * 4 + x}
        )

    def ax_copy(h, qi, j):
        src = att.at[qi, lax.rem(x + j, 4), :, pl.ds(pl.multiple_of(h * HD, HD), HD)]
        there = pl.ds(pl.multiple_of((4 - j) * F + h * HD, HD), HD)
        return remote(
            src, gat.at[0, qi, :, there], ax_send.at[h, j - 1], ax_recv.at[h, 3 - j], along(0, j)
        )

    def ax_all(h, k):
        part = gat.at[0, :, :, pl.ds(h * HD, HD)]
        return remote(part, part, ax_send.at[h, k - 1], ax_recv.at[h, k - 1], along(0, k))

    def head(h, carry):
        col = pl.multiple_of(h * HD, HD)
        for qi in range(LEN // BQ):
            for half in range(BQ // RC):
                top_row = qi * BQ + half * RC
                kv = -(-(top_row + RC) // HD) * HD
                q = qkv[top_row : top_row + RC, pl.ds(col, HD)]
                limit = jnp.minimum(lax.broadcasted_iota(jnp.int32, (RC, 1), 0) + top_row, last)
                tiles = [(lo, min(lo + 256, kv)) for lo in range(0, kv, 256)]
                most = None
                for lo, hi in tiles:
                    k = qkv[lo:hi, pl.ds(F + col, HD)]
                    sc = lax.dot_general(q, k, (((1,), (1,)), ((), ())), preferred_element_type=jnp.float32)
                    if hi > min(top_row + 1, LEN // 2 + 1):
                        sc = jnp.where(lax.broadcasted_iota(jnp.int32, (RC, hi - lo), 1) + lo <= limit, sc, -1e30)
                    sbuf[:, lo:hi] = sc
                    for t in range(0, hi - lo, HD):
                        most = sc[:, t : t + HD] if most is None else jnp.maximum(most, sc[:, t : t + HD])
                top = jnp.max(most, axis=-1, keepdims=True) * SCALE2
                total = None
                for t in range(0, kv, HD):
                    e = jnp.exp2(sbuf[:, t : t + HD] * SCALE2 - top)
                    total = e if total is None else total + e
                top = top + jnp.log2(jnp.sum(total, axis=-1, keepdims=True))
                o = None
                for lo, hi in tiles:
                    p = jnp.exp2(sbuf[:, lo:hi] * SCALE2 - top).astype(jnp.bfloat16)
                    part = jnp.dot(p, qkv[lo:hi, pl.ds(2 * F + col, HD)], preferred_element_type=jnp.float32)
                    o = part if o is None else o + part
                att[qi, 2 * half : 2 * half + 2, :, pl.ds(col, HD)] = o.astype(jnp.bfloat16).reshape(2, ROWS, HD)
            for j in (2, 1, 3):
                ax_copy(h, qi, j).start()

            @pl.when(z != qi)
            def _():
                az_copy(h, qi, lax.rem(z - qi + 4, 4)).start()

        @pl.when(h == 0)
        def _():
            for axis, k in blocks:
                gd_copy(axis, k).wait_recv()
            for n in range(CHUNKS):
                for k in range(4):
                    load(n, k).start()

        return carry

    lax.fori_loop(0, HEADS, head, 0)
    for b in range(4):
        gat[0, b, :, 0:F] = att[b, x]
        gat[1, b, :, 0:F] = att[z, b]

    for h in range(HEADS):
        for k in (1, 2, 3):
            az_copy(h, 0, k).wait_recv()
            ax_all(h, k).wait_recv()

    def out_copy(n):
        lo = (n % 2) * HC + (n // 2) * CW
        return pltpu.make_async_copy(out.at[n], out_ref.at[:, pl.ds(lo, CW)], out_sem.at[n])

    def p_copy(n, what):
        axis, ahead = 1 - n % 2, (1 if (n // 2) % 2 == 0 else 3)
        here = x if axis == 0 else z
        j = (ahead, ahead, 4 - ahead)[what]
        block = lax.rem(here + (2 if what == 0 else j), 4)
        return remote(
            psend.at[n, block], prec.at[n, what], p_send.at[n],
            p0_recv.at[n] if what == 0 else p_recv.at[n], along(axis, j),
        )

    def p_all(n, count):
        part = prec.at[n, pl.ds(0, count)]
        return remote(part, part, p_send.at[n], p_recv.at[n], along(0, 1))

    def p_add(n):
        axis, ahead = 1 - n % 2, (1 if (n // 2) % 2 == 0 else 3)
        block = lax.rem((x if axis == 0 else z) + ahead, 4)
        p_copy(n, 0).wait_recv()
        both = psend[n, block].astype(jnp.float32) + prec[n, 0].astype(jnp.float32)
        psend[n, block] = both.astype(jnp.bfloat16)
        p_copy(n, 1).start()

    for n in range(CHUNKS):
        ref, row, col = home_of(n)
        loaded(n).wait()
        a = gat[n % 2].reshape(4 * ROWS, KX)
        res = jnp.dot(a, ref[row : row + KX, col : col + CW], preferred_element_type=jnp.float32)
        psend[n] = res.astype(jnp.bfloat16).reshape(4, ROWS, CW)
        p_copy(n, 0).start()
        p_copy(n, 2).start()
        if n >= LAG:
            p_add(n - LAG)
    for n in range(CHUNKS - LAG, CHUNKS):
        p_add(n)

    for n in range(CHUNKS):
        here = z if n % 2 == 0 else x
        lo = (n % 2) * HC + (n // 2) * CW
        total = psend[n, here].astype(jnp.float32) + bo_ref[:, lo : lo + CW]
        p_all(n, 2).wait_recv()
        total += prec[n, 1].astype(jnp.float32) + prec[n, 2].astype(jnp.float32)
        out[n] = total.astype(jnp.bfloat16)
        out_copy(n).start()

    for n in range(CHUNKS):
        p_all(n, 3).wait_send()
    for i, sent in enumerate(
        (
            g_hbm.at[0, 0, pl.ds(0, 4 * PR)],
            g_hbm.at[0, 0, pl.ds(0, 2 * PR)],
            g_hbm.at[0, 0, pl.ds(0, 6 * PR)],
            g_hbm.at[0, 0, pl.ds(0, 6 * PR)],
            g_hbm.at[0, 0, pl.ds(0, 6 * PR)],
            g_hbm.at[0],
        )
    ):
        remote(sent, sent, g_send.at[i], gd_recv.at[0, 0], sibling).wait_send()
    for h in range(HEADS):
        for k in (1, 2, 3):
            az_copy(h, 0, k).wait_send()
            ax_all(h, k).wait_send()
    for n in range(CHUNKS):
        out_copy(n).wait()
    kv_copy.wait()


def finish_kernel(page_ref, len_ref, part_hbm, new_hbm, old_hbm, out_hbm, kv_hbm, part, new, kv, in_sem, out_sem):
    group = SLOTS * PAGE // 4
    news = [
        pltpu.make_async_copy(new_hbm.at[pl.ds(g * BQ, BQ)], new.at[pl.ds(g * BQ, BQ)], in_sem.at[g])
        for g in range(4)
    ]
    olds = [
        pltpu.make_async_copy(
            old_hbm.at[:, pl.ds(g * group, group)], kv.at[:, pl.ds(g * group, group)], in_sem.at[4 + g]
        )
        for g in range(4)
    ]
    kvs = [
        pltpu.make_async_copy(
            kv.at[:, pl.ds(g * group, group)], kv_hbm.at[:, pl.ds(g * group, group)], out_sem.at[g]
        )
        for g in range(4)
    ]
    load = pltpu.make_async_copy(part_hbm, part, in_sem.at[8])
    store = pltpu.make_async_copy(part, out_hbm, out_sem.at[4])
    for copy in [*news, *olds, load]:
        copy.start()
    for copy in news:
        copy.wait()
    for g in range(4):
        olds[g].wait()
        for i in range(g * SLOTS // 4, (g + 1) * SLOTS // 4):
            page = jnp.int32(-1)
            for p in range(PAGES):
                page = jnp.where(page_ref[0, p] == i, p, page)
            row = lax.broadcasted_iota(jnp.int32, (PAGE, 1), 0) + page * PAGE
            written = (row < len_ref[0]) & (row >= 0)
            rows = pl.ds(pl.multiple_of(jnp.maximum(page, 0) * PAGE, PAGE), PAGE)
            for c in range(2):
                old = kv[c, i * PAGE : (i + 1) * PAGE, :]
                kv[c, i * PAGE : (i + 1) * PAGE, :] = jnp.where(written, new[rows, c * F : (c + 1) * F], old)
        kvs[g].start()
    load.wait()
    store.start()
    for copy in [*kvs, store]:
        copy.wait()


def body(tokens, ln_gain, ln_bias, w_qkv, b_qkv, w_out, b_out, kv_cache, page_table, lengths):
    vmem = pl.BlockSpec(memory_space=pltpu.VMEM)
    anym = pl.BlockSpec(memory_space=pl.ANY)
    smem = pl.BlockSpec(memory_space=pltpu.SMEM)
    dma = pltpu.SemaphoreType.DMA
    part, kv_new, _ = pl.pallas_call(
        main_kernel,
        out_shape=(
            jax.ShapeDtypeStruct((ROWS, D), jnp.bfloat16),
            jax.ShapeDtypeStruct((LEN, 2 * F), jnp.bfloat16),
            jax.ShapeDtypeStruct((2, 3, F, HC), jnp.bfloat16),
        ),
        in_specs=[smem, vmem, vmem, vmem, anym, vmem, anym, vmem],
        out_specs=(anym, anym, anym),
        scratch_shapes=[
            pltpu.VMEM((RINGS, SUBS, LEN, CW), jnp.bfloat16),
            pltpu.VMEM((D, 3 * F), jnp.bfloat16),
            pltpu.VMEM((LEN, 3 * F), jnp.float32),
            pltpu.VMEM((LEN, 3 * F), jnp.bfloat16),
            pltpu.VMEM((4, 4, ROWS, F), jnp.bfloat16),
            pltpu.VMEM((KX, 4 * CW), jnp.bfloat16),
            pltpu.VMEM((2, 4, ROWS, KX), jnp.bfloat16),
            pltpu.VMEM((CHUNKS, 4, ROWS, CW), jnp.bfloat16),
            pltpu.VMEM((CHUNKS, 3, ROWS, CW), jnp.bfloat16),
            pltpu.VMEM((RC, LEN), jnp.float32),
            pltpu.VMEM((CHUNKS, ROWS, CW), jnp.bfloat16),
            dma((RINGS, SUBS)),
            dma((RINGS, SUBS, SPAN)),
            dma,
            dma,
            dma((CHUNKS,)),
            dma((6,)),
            dma((2, 2)),
            dma((2, 2)),
            dma((2, 3, 2)),
            dma((2, 3)),
            dma((2, 3)),
            dma((CHUNKS,)),
            dma((HEADS, 3)),
            dma((HEADS, 3)),
            dma((HEADS, 3)),
            dma((HEADS, 3)),
            dma((CHUNKS,)),
            dma((CHUNKS,)),
            dma((CHUNKS,)),
        ],
        compiler_params=pltpu.CompilerParams(
            collective_id=0, has_side_effects=True, vmem_limit_bytes=67043328
        ),
        name="sublayer",
    )(
        lengths,
        tokens,
        ln_gain.reshape(1, D),
        ln_bias.reshape(1, D),
        jnp.transpose(w_qkv, (1, 0, 2)),
        b_qkv,
        w_out,
        b_out.reshape(1, D),
    )
    out, kv_out = pl.pallas_call(
        finish_kernel,
        out_shape=(
            jax.ShapeDtypeStruct((ROWS, D), jnp.bfloat16),
            jax.ShapeDtypeStruct((2, SLOTS * PAGE, F), jnp.bfloat16),
        ),
        in_specs=[smem, smem, anym, anym, anym],
        out_specs=(anym, anym),
        scratch_shapes=[
            pltpu.VMEM((ROWS, D), jnp.bfloat16),
            pltpu.VMEM((LEN, 2 * F), jnp.bfloat16),
            pltpu.VMEM((2, SLOTS * PAGE, F), jnp.bfloat16),
            dma((9,)),
            dma((5,)),
        ],
        name="finish",
    )(page_table, lengths, part, kv_new, kv_cache.reshape(2, SLOTS * PAGE, F))
    return out, kv_out.reshape(kv_cache.shape)


def solution(mesh):
    placed = (
        P(("dp", "tp"), None),
        P(),
        P(),
        P(None, None, "tp"),
        P(None, "tp"),
        P("tp", None),
        P(),
        P(None, "dp", None, "tp"),
        P("dp", None),
        P("dp"),
    )
    return jax.shard_map(
        body,
        mesh=mesh,
        in_specs=placed,
        out_specs=(P(("dp", "tp"), None), P(None, "dp", None, "tp")),
        check_vma=False,
    )
```

```python
import functools

import jax
import jax.numpy as jnp
from jax import lax
from jax.experimental import pallas as pl
from jax.experimental.pallas import tpu as pltpu
from jax.sharding import PartitionSpec as P

HD = 128
EPS = 1e-05
MESH = pl.DeviceIdType.MESH
RINGS = 4
SUBS = 3
N = 16
ROWS = 80
CW = 512
QW = SUBS * CW
D = RINGS * QW
LEN = N * ROWS
F = 384
HEADS = F // HD
BQ = 320
BATCH = 4
PAGE = 128
PAGES = LEN // PAGE
SLOTS = 12
HC = D // 2
PR = F // 8
KX = 4 * F
CHUNKS = 12
LAG = 4
QB = 128
PIECES = ((0, 320, 0), (320, 640, 1), (640, 960, 2), (960, 1152, 3), (1152, 1280, 3))
SPAN = 4
FORWARD_AT = 4
SCALE2 = 1.4426950408889634 / (HD ** 0.5)


def ring_tp(ring, pos):
    a = lax.div(pos, 4)
    b = lax.rem(lax.rem(pos, 4) - a + 4, 4)
    return jnp.where(ring < 2, a * 4 + b, b * 4 + a)


def my_pos(ring, z, x):
    t = lax.rem(z + x, 4)
    return jnp.where(ring < 2, 4 * z + t, 4 * x + t)


def behind(ring, pos, k):
    up = lax.rem(ring, 2)
    return lax.rem(jnp.where(up == 0, pos + N - k, pos + k), N)


def main_kernel(
    len_ref, tok_ref, gain_ref, shift_ref, w_hbm, bq_ref, wo_hbm, bo_ref,
    out_ref, kv_hbm, g_hbm,
    ag, w, acc, qkv, att, wx, gat, psend, prec, out,
    ag_send, ag_recv, w_sem, kv_sem, out_sem,
    g_send, g1_recv, g2_recv, gy_recv, gf_recv, gd_recv,
    l_sem, az_send, az_recv, ax_send, ax_recv, p_send, p0_recv, p_recv,
):
    tp = lax.axis_index("tp")
    dp = lax.axis_index("dp")
    z = lax.div(tp, 4)
    x = lax.rem(tp, 4)
    y = lax.div(dp, 2)
    core = lax.rem(dp, 2)
    pos = [my_pos(jnp.int32(r), z, x) for r in range(RINGS)]
    nxt = [ring_tp(jnp.int32(r), behind(jnp.int32(r), pos[r], N - 1)) for r in range(RINGS)]

    def along(axis, j):
        if axis == 0:
            return {"tp": z * 4 + lax.rem(x + j, 4)}
        return {"tp": lax.rem(z + j, 4) * 4 + x}

    def along_y(j):
        return {"dp": lax.rem(y + j, 4) * 2 + core}

    sibling = {"dp": y * 2 + 1 - core}

    barrier = pltpu.get_barrier_semaphore()
    peers = [along(a, j) for a in range(2) for j in (1, 2, 3)] + [along_y(1), along_y(3), sibling]
    for peer in peers:
        pl.semaphore_signal(barrier, inc=1, device_id=peer, device_id_type=MESH)

    w_copies = [
        pltpu.make_async_copy(w_hbm.at[c], w.at[:, pl.ds(c * F, F)], w_sem) for c in range(3)
    ]
    for copy in w_copies:
        copy.start()
    pl.semaphore_wait(barrier, len(peers))

    def remote(src, dst, send_sem, recv_sem, device):
        return pltpu.make_async_remote_copy(
            src_ref=src, dst_ref=dst, send_sem=send_sem, recv_sem=recv_sem,
            device_id=device, device_id_type=MESH,
        )

    piece = pl.ds(pl.multiple_of((core * 4 + y) * PR, PR), PR)

    def g1_copy(axis, j):
        return remote(
            wo_hbm.at[piece, pl.ds(axis * HC, HC)], g_hbm.at[axis, 3 - j, piece],
            g_send.at[0], g1_recv.at[axis, j // 2], along(axis, j),
        )

    def g2_copy(axis, j):
        k = 4 - j
        cols = pl.ds(0 if j == 1 else HC // 2, HC // 2)
        return remote(
            g_hbm.at[axis, k - 1, piece, cols], g_hbm.at[axis, 1, piece, cols],
            g_send.at[1], g2_recv.at[axis, j // 2], along(axis, j),
        )

    for axis in range(2):
        for j in (1, 3):
            g1_copy(axis, j).start()

    def norm_rows(i, carry):
        rows = pl.ds(pl.multiple_of(i * 16, 16), 16)
        v = tok_ref[rows, :].astype(jnp.float32)
        center = jnp.mean(v, axis=-1, keepdims=True)
        v = v - center
        spread = jnp.mean(v * v, axis=-1, keepdims=True)
        v = (v * lax.rsqrt(spread + EPS) * gain_ref[...] + shift_ref[...]).astype(jnp.bfloat16)
        for r in range(RINGS):
            for c in range(SUBS):
                ag[r, c, rows, :] = v[:, r * QW + c * CW : r * QW + (c + 1) * CW]
        return carry

    lax.fori_loop(0, ROWS // 16, norm_rows, 0)

    def slot(s):
        if isinstance(s, int):
            return pl.ds(s * ROWS, ROWS)
        return pl.ds(pl.multiple_of(s * ROWS, 16), ROWS)

    def ag_copy(r, c, s):
        return remote(
            ag.at[r, c, slot(s)], ag.at[r, c, slot(s + 1)],
            ag_send.at[r, c], ag_recv.at[r, c, lax.rem(s + 1, SPAN)], {"tp": nxt[r]},
        )

    def ag_arrived(r, c, s):
        return remote(
            ag.at[r, c, slot(s)], ag.at[r, c, slot(s)],
            ag_send.at[r, c], ag_recv.at[r, c, lax.rem(s, SPAN)], {"tp": nxt[r]},
        )

    for r in range(RINGS):
        ag_copy(r, 0, 0).start()
    for j in (1, 3):
        for axis in range(2):
            g1_copy(axis, j).wait_recv()
            g2_copy(axis, j).start()
    for c in range(1, SUBS):
        for r in range(RINGS):
            ag_copy(r, c, 0).start()

    for c in range(3):
        acc[:, c * F : (c + 1) * F] = jnp.broadcast_to(bq_ref[c : c + 1, :], (LEN, F))
    pltpu.make_async_copy(w, w, w_sem).wait()

    def gy_copy(axis, k, j):
        return remote(
            g_hbm.at[axis, k - 1, piece], g_hbm.at[axis, k - 1, piece],
            g_send.at[2 + axis], gy_recv.at[axis, k - 1, j // 2], along_y(j),
        )

    def gf_copy(axis, k):
        j = 1 if axis == 0 else 3
        src = pl.ds(pl.multiple_of((core * 4 + lax.rem(y + 4 - j, 4)) * PR, PR), PR)
        return remote(
            g_hbm.at[axis, k - 1, src], g_hbm.at[axis, k - 1, src],
            g_send.at[4], gf_recv.at[axis, k - 1], along_y(j),
        )

    for k in (1, 3, 2):
        if k == 2:
            for axis in range(2):
                for j in (1, 3):
                    g2_copy(axis, j).wait_recv()
        for axis in range(2):
            gy_copy(axis, k, 1 if axis == 0 else 3).start()
    for k in (1, 3, 2):
        for axis in range(2):
            gy_copy(axis, k, 3 if axis == 0 else 1).start()

    def unit(first, count, r, subs, cols):
        home = jnp.where(r < 2, 4 * z, 4 * x) + lax.rem(z + x, 4)
        rows = pl.ds(pl.multiple_of(first * ROWS, 16), count * ROWS)
        for lo, hi in cols:
            res = None
            for c in subs:
                wrow = pl.ds(pl.multiple_of(r * QW + c * CW, CW), CW)
                part = jnp.dot(ag[r, c, rows, :], w[wrow, lo:hi], preferred_element_type=jnp.float32)
                res = part if res is None else res + part
            for i in range(count):
                src = ring_tp(r, behind(r, home, first + i))
                to = pl.ds(pl.multiple_of(src * ROWS, 16), ROWS)
                acc[to, lo:hi] += res[i * ROWS : (i + 1) * ROWS]

    halves, whole = ((0, 640), (640, 1152)), ((0, 1152),)

    mine = pl.ds(pl.multiple_of(core * (4 * PR), 4 * PR), 4 * PR)

    def gd_copy(axis, k):
        return remote(
            g_hbm.at[axis, k - 1, mine], g_hbm.at[axis, k - 1, mine],
            g_send.at[5], gd_recv.at[axis, k - 1], sibling,
        )

    blocks = [(axis, k) for axis in range(2) for k in (1, 2, 3)]

    def ag_step(s, carry):
        first = jnp.where(s < 12, s - 4, 2 * s - 16)
        count = jnp.where(s < 4, 0, jnp.where(s < 12, 1, jnp.where(s < 14, 2, 0)))
        for c in range(SUBS):
            for r in range(RINGS):
                ag_arrived(r, c, s).wait_recv()
                ag_copy(r, c, s - 1).wait_send()
                ag_copy(r, c, s).start()

            def four(u, carry, c=c):
                unit(lax.div(u, RINGS) * 4, 4, lax.rem(u, RINGS), (c,), halves)
                return carry

            lax.fori_loop(first, first + count, four, 0)

        for i, k in enumerate((1, 3, 2)):

            @pl.when(s == FORWARD_AT + i)
            def _():
                for axis in range(2):
                    gy_copy(axis, k, 1 if axis == 0 else 3).wait_recv()
                    gf_copy(axis, k).start()

        @pl.when(s == 13)
        def _():
            for axis, k in blocks:
                gy_copy(axis, k, 3 if axis == 0 else 1).wait_recv()
                gf_copy(axis, k).wait_recv()
                gd_copy(axis, k).start()

        return carry

    lax.fori_loop(1, N - 1, ag_step, 0)

    def two(first):
        def step(r, carry):
            unit(first, 2, r, (0, 1, 2), whole)
            return carry

        lax.fori_loop(0, RINGS, step, 0)

    two(12)
    for c in range(SUBS):
        for r in range(RINGS):
            ag_arrived(r, c, N - 1).wait_recv()
            ag_copy(r, c, N - 2).wait_send()
    two(14)

    def to_bf16(i, carry):
        rows = pl.ds(pl.multiple_of(i * 64, 64), 64)
        qkv[rows, :] = acc[rows, :].astype(jnp.bfloat16)
        return carry

    lax.fori_loop(0, LEN // 64, to_bf16, 0)

    kv_copy = pltpu.make_async_copy(qkv.at[:, pl.ds(F, 2 * F)], kv_hbm, kv_sem)
    kv_copy.start()

    def home_of(n):
        if n < 8:
            return w, (n // 2) * KX, (n % 2) * CW
        return wx, 0, (n - 8) * CW

    def load(n, k):
        axis, m = n % 2, n // 2
        ref, row, col = home_of(n)
        if k == 0:
            src = wo_hbm.at[:, pl.ds(axis * HC + m * CW, CW)]
        else:
            src = g_hbm.at[axis, k - 1, :, pl.ds(m * CW, CW)]
        return pltpu.make_async_copy(src, ref.at[pl.ds(row + k * F, F), pl.ds(col, CW)], l_sem.at[n])

    def loaded(n):
        ref, row, col = home_of(n)
        chunk = ref.at[pl.ds(row, KX), pl.ds(col, CW)]
        return pltpu.make_async_copy(chunk, chunk, l_sem.at[n])

    last = len_ref[0] - 1

    def az_copy(h, lo, hi, qi, k):
        src = att.at[pl.ds(lo, hi - lo), pl.ds(pl.multiple_of(h * HD, HD), HD)]
        there = pl.ds(pl.multiple_of(k * F + h * HD, HD), HD)
        return remote(
            src, gat.at[1, pl.ds(lo - qi * BQ, hi - lo), there],
            az_send.at[h], az_recv.at[h, k - 1], {"tp": qi * 4 + x},
        )

    def ax_copy(h, qi, j):
        block = pl.ds(pl.multiple_of((4 * qi + lax.rem(x + j, 4)) * ROWS, 16), ROWS)
        src = att.at[block, pl.ds(pl.multiple_of(h * HD, HD), HD)]
        there = pl.ds(pl.multiple_of((4 - j) * F + h * HD, HD), HD)
        return remote(
            src, gat.at[0, pl.ds(qi * ROWS, ROWS), there], ax_send.at[h], ax_recv.at[h, 3 - j], along(0, j)
        )

    def a_all(axis, h, k):
        part = gat.at[axis, :, pl.ds(h * HD, HD)]
        sends, recvs = ((ax_send, ax_recv), (az_send, az_recv))[axis]
        return remote(part, part, sends.at[h], recvs.at[h, k - 1], along(axis, k))

    def a_sent(axis, h):
        part = gat.at[axis, :, pl.ds(0, 3 * HD)]
        return remote(part, part, (ax_send, az_send)[axis].at[h], ax_recv.at[h, 0], along(0, 1))

    def head(h, carry):
        col = pl.multiple_of(h * HD, HD)
        for row in range(0, LEN, QB):
            kv = row + QB
            free = min(row, LEN // 2)
            q = qkv[row : row + QB, pl.ds(col, HD)]
            k = qkv[0:kv, pl.ds(F + col, HD)]
            v = qkv[0:kv, pl.ds(2 * F + col, HD)]
            sc = lax.dot_general(k, q, (((1,), (1,)), ((), ())), preferred_element_type=jnp.float32)
            limit = jnp.minimum(lax.broadcasted_iota(jnp.int32, (1, QB), 1) + row, last)
            key = lax.broadcasted_iota(jnp.int32, (kv - free, QB), 0) + free
            masked = jnp.where(key <= limit, sc[free:], -1e30)
            sc = jnp.concatenate([sc[:free], masked], axis=0) if free else masked
            top = jnp.max(sc, axis=0, keepdims=True)
            e = jnp.exp2((sc - top) * SCALE2)
            inv = 1.0 / jnp.sum(e, axis=0, keepdims=True)
            p = (e * inv).astype(jnp.bfloat16)
            o = lax.dot_general(p, v, (((0,), (0,)), ((), ())), preferred_element_type=jnp.float32)
            att[row : row + QB, pl.ds(col, HD)] = o.astype(jnp.bfloat16)
            for lo, hi, qi in PIECES:
                if row < hi <= kv:

                    @pl.when(z != qi)
                    def _():
                        az_copy(h, lo, hi, qi, lax.rem(z - qi + 4, 4)).start()

                    if hi == (qi + 1) * BQ:
                        for j in (2, 1, 3):
                            ax_copy(h, qi, j).start()

        @pl.when(h == 0)
        def _():
            for axis, k in blocks:
                gd_copy(axis, k).wait_recv()
            for n in range(CHUNKS):
                for k in range(4):
                    load(n, k).start()

        return carry

    lax.fori_loop(0, HEADS, head, 0)
    for b in range(4):
        gat[0, b * ROWS : (b + 1) * ROWS, 0:F] = att[pl.ds(pl.multiple_of((4 * b + x) * ROWS, 16), ROWS), :]
    gat[1, :, 0:F] = att[pl.ds(pl.multiple_of(z * BQ, 64), BQ), :]

    def out_copy(n):
        lo = (n % 2) * HC + (n // 2) * CW
        return pltpu.make_async_copy(out.at[n], out_ref.at[:, pl.ds(lo, CW)], out_sem.at[n])

    def p_copy(n, what):
        axis, ahead = 1 - n % 2, (1 if (n // 2) % 2 == 0 else 3)
        here = x if axis == 0 else z
        j = (ahead, ahead, 4 - ahead)[what]
        block = lax.rem(here + (2 if what == 0 else j), 4)
        return remote(
            psend.at[n, block], prec.at[n, what], p_send.at[n],
            p0_recv.at[n] if what == 0 else p_recv.at[n], along(axis, j),
        )

    def p_all(n, count):
        part = prec.at[n, pl.ds(0, count)]
        return remote(part, part, p_send.at[n], p_recv.at[n], along(0, 1))

    def p_add(n):
        axis, ahead = 1 - n % 2, (1 if (n // 2) % 2 == 0 else 3)
        block = lax.rem((x if axis == 0 else z) + ahead, 4)
        p_copy(n, 0).wait_recv()
        both = psend[n, block].astype(jnp.float32) + prec[n, 0].astype(jnp.float32)
        psend[n, block] = both.astype(jnp.bfloat16)
        p_copy(n, 1).start()

    for n in range(CHUNKS):
        ref, row, col = home_of(n)
        if n < 2:
            for h in range(HEADS):
                for k in (1, 2, 3):
                    a_all(n, h, k).wait_recv()
        loaded(n).wait()
        res = jnp.dot(gat[n % 2], ref[row : row + KX, col : col + CW], preferred_element_type=jnp.float32)
        psend[n] = res.astype(jnp.bfloat16).reshape(4, ROWS, CW)
        p_copy(n, 0).start()
        p_copy(n, 2).start()
        if n >= LAG:
            p_add(n - LAG)
    for n in range(CHUNKS - LAG, CHUNKS):
        p_add(n)

    for n in range(CHUNKS):
        here = z if n % 2 == 0 else x
        lo = (n % 2) * HC + (n // 2) * CW
        total = psend[n, here].astype(jnp.float32) + bo_ref[:, lo : lo + CW]
        p_all(n, 2).wait_recv()
        total += prec[n, 1].astype(jnp.float32) + prec[n, 2].astype(jnp.float32)
        out[n] = total.astype(jnp.bfloat16)
        out_copy(n).start()

    for n in range(CHUNKS):
        p_all(n, 3).wait_send()
    for i, sent in enumerate(
        (
            g_hbm.at[0, 0, pl.ds(0, 4 * PR)],
            g_hbm.at[0, 0, pl.ds(0, 2 * PR)],
            g_hbm.at[0, 0, pl.ds(0, 6 * PR)],
            g_hbm.at[0, 0, pl.ds(0, 6 * PR)],
            g_hbm.at[0, 0, pl.ds(0, 6 * PR)],
            g_hbm.at[0],
        )
    ):
        remote(sent, sent, g_send.at[i], gd_recv.at[0, 0], sibling).wait_send()
    for h in range(HEADS):
        for axis in range(2):
            a_sent(axis, h).wait_send()
    for n in range(CHUNKS):
        out_copy(n).wait()
    kv_copy.wait()


def finish_kernel(page_ref, len_ref, part_hbm, new_hbm, old_hbm, out_hbm, kv_hbm, part, new, kv, in_sem, out_sem):
    group = SLOTS * PAGE // 4
    news = [
        pltpu.make_async_copy(new_hbm.at[pl.ds(g * BQ, BQ)], new.at[pl.ds(g * BQ, BQ)], in_sem.at[g])
        for g in range(4)
    ]
    olds = [
        pltpu.make_async_copy(
            old_hbm.at[:, pl.ds(g * group, group)], kv.at[:, pl.ds(g * group, group)], in_sem.at[4 + g]
        )
        for g in range(4)
    ]
    kvs = [
        pltpu.make_async_copy(
            kv.at[:, pl.ds(g * group, group)], kv_hbm.at[:, pl.ds(g * group, group)], out_sem.at[g]
        )
        for g in range(4)
    ]
    load = pltpu.make_async_copy(part_hbm, part, in_sem.at[8])
    store = pltpu.make_async_copy(part, out_hbm, out_sem.at[4])
    for copy in [*news, *olds, load]:
        copy.start()
    for copy in news:
        copy.wait()
    for g in range(4):
        olds[g].wait()
        for i in range(g * SLOTS // 4, (g + 1) * SLOTS // 4):
            page = jnp.int32(-1)
            for p in range(PAGES):
                page = jnp.where(page_ref[0, p] == i, p, page)
            row = lax.broadcasted_iota(jnp.int32, (PAGE, 1), 0) + page * PAGE
            written = (row < len_ref[0]) & (row >= 0)
            rows = pl.ds(pl.multiple_of(jnp.maximum(page, 0) * PAGE, PAGE), PAGE)
            for c in range(2):
                old = kv[c, i * PAGE : (i + 1) * PAGE, :]
                kv[c, i * PAGE : (i + 1) * PAGE, :] = jnp.where(written, new[rows, c * F : (c + 1) * F], old)
        kvs[g].start()
    load.wait()
    store.start()
    for copy in [*kvs, store]:
        copy.wait()


def body(tokens, ln_gain, ln_bias, w_qkv, b_qkv, w_out, b_out, kv_cache, page_table, lengths):
    vmem = pl.BlockSpec(memory_space=pltpu.VMEM)
    anym = pl.BlockSpec(memory_space=pl.ANY)
    smem = pl.BlockSpec(memory_space=pltpu.SMEM)
    dma = pltpu.SemaphoreType.DMA
    part, kv_new, _ = pl.pallas_call(
        main_kernel,
        out_shape=(
            jax.ShapeDtypeStruct((ROWS, D), jnp.bfloat16),
            jax.ShapeDtypeStruct((LEN, 2 * F), jnp.bfloat16),
            jax.ShapeDtypeStruct((2, 3, F, HC), jnp.bfloat16),
        ),
        in_specs=[smem, vmem, vmem, vmem, anym, vmem, anym, vmem],
        out_specs=(anym, anym, anym),
        scratch_shapes=[
            pltpu.VMEM((RINGS, SUBS, LEN, CW), jnp.bfloat16),
            pltpu.VMEM((D, 3 * F), jnp.bfloat16),
            pltpu.VMEM((LEN, 3 * F), jnp.float32),
            pltpu.VMEM((LEN, 3 * F), jnp.bfloat16),
            pltpu.VMEM((LEN, F), jnp.bfloat16),
            pltpu.VMEM((KX, 4 * CW), jnp.bfloat16),
            pltpu.VMEM((2, BQ, KX), jnp.bfloat16),
            pltpu.VMEM((CHUNKS, 4, ROWS, CW), jnp.bfloat16),
            pltpu.VMEM((CHUNKS, 3, ROWS, CW), jnp.bfloat16),
            pltpu.VMEM((CHUNKS, ROWS, CW), jnp.bfloat16),
            dma((RINGS, SUBS)),
            dma((RINGS, SUBS, SPAN)),
            dma,
            dma,
            dma((CHUNKS,)),
            dma((6,)),
            dma((2, 2)),
            dma((2, 2)),
            dma((2, 3, 2)),
            dma((2, 3)),
            dma((2, 3)),
            dma((CHUNKS,)),
            dma((HEADS,)),
            dma((HEADS, 3)),
            dma((HEADS,)),
            dma((HEADS, 3)),
            dma((CHUNKS,)),
            dma((CHUNKS,)),
            dma((CHUNKS,)),
        ],
        compiler_params=pltpu.CompilerParams(
            collective_id=0, has_side_effects=True, vmem_limit_bytes=67043328
        ),
        name="sublayer",
    )(
        lengths,
        tokens,
        ln_gain.reshape(1, D),
        ln_bias.reshape(1, D),
        jnp.transpose(w_qkv, (1, 0, 2)),
        b_qkv,
        w_out,
        b_out.reshape(1, D),
    )
    out, kv_out = pl.pallas_call(
        finish_kernel,
        out_shape=(
            jax.ShapeDtypeStruct((ROWS, D), jnp.bfloat16),
            jax.ShapeDtypeStruct((2, SLOTS * PAGE, F), jnp.bfloat16),
        ),
        in_specs=[smem, smem, anym, anym, anym],
        out_specs=(anym, anym),
        scratch_shapes=[
            pltpu.VMEM((ROWS, D), jnp.bfloat16),
            pltpu.VMEM((LEN, 2 * F), jnp.bfloat16),
            pltpu.VMEM((2, SLOTS * PAGE, F), jnp.bfloat16),
            dma((9,)),
            dma((5,)),
        ],
        name="finish",
    )(page_table, lengths, part, kv_new, kv_cache.reshape(2, SLOTS * PAGE, F))
    return out, kv_out.reshape(kv_cache.shape)


def solution(mesh):
    placed = (
        P(("dp", "tp"), None),
        P(),
        P(),
        P(None, None, "tp"),
        P(None, "tp"),
        P("tp", None),
        P(),
        P(None, "dp", None, "tp"),
        P("dp", None),
        P("dp"),
    )
    return jax.shard_map(
        body,
        mesh=mesh,
        in_specs=placed,
        out_specs=(P(("dp", "tp"), None), P(None, "dp", None, "tp")),
        check_vma=False,
    )
```

```python
import functools

import jax
import jax.numpy as jnp
from jax import lax
from jax.experimental import pallas as pl
from jax.experimental.pallas import tpu as pltpu
from jax.sharding import PartitionSpec as P

HD = 128
EPS = 1e-05
MESH = pl.DeviceIdType.MESH
RINGS = 4
SUBS = 3
N = 16
ROWS = 80
CW = 512
QW = SUBS * CW
D = RINGS * QW
LEN = N * ROWS
F = 384
HEADS = F // HD
BQ = 320
BATCH = 4
PAGE = 128
PAGES = LEN // PAGE
SLOTS = 12
HC = D // 2
PR = F // 8
KX = 4 * F
CHUNKS = 12
LAG = 4
QB = 256
SPAN = 4
FORWARD_AT = 4
SCALE2 = 1.4426950408889634 / (HD ** 0.5)


def ring_tp(ring, pos):
    a = lax.div(pos, 4)
    b = lax.rem(lax.rem(pos, 4) - a + 4, 4)
    return jnp.where(ring < 2, a * 4 + b, b * 4 + a)


def my_pos(ring, z, x):
    t = lax.rem(z + x, 4)
    return jnp.where(ring < 2, 4 * z + t, 4 * x + t)


def behind(ring, pos, k):
    up = lax.rem(ring, 2)
    return lax.rem(jnp.where(up == 0, pos + N - k, pos + k), N)


def main_kernel(
    len_ref, tok_hbm, gain_hbm, shift_hbm, w_hbm, bq_hbm, wo_hbm, bo_hbm,
    out_ref, kv_hbm, g_hbm,
    ag, w, acc, qkv, att, wx, gat, psend, prec, out,
    tok_ref, gain_ref, shift_ref, bq_ref, bo_ref, in_sem,
    ag_send, ag_recv, w_sem, kv_sem, out_sem,
    g_send, g1_recv, g2_recv, gy_recv, gf_recv, gd_recv,
    l_sem, az_send, az_recv, ax_send, ax_recv, p_send, p0_recv, p_recv,
):
    tp = lax.axis_index("tp")
    dp = lax.axis_index("dp")
    z = lax.div(tp, 4)
    x = lax.rem(tp, 4)
    y = lax.div(dp, 2)
    core = lax.rem(dp, 2)
    pos = [my_pos(jnp.int32(r), z, x) for r in range(RINGS)]
    nxt = [ring_tp(jnp.int32(r), behind(jnp.int32(r), pos[r], N - 1)) for r in range(RINGS)]

    def along(axis, j):
        if axis == 0:
            return {"tp": z * 4 + lax.rem(x + j, 4)}
        return {"tp": lax.rem(z + j, 4) * 4 + x}

    def along_y(j):
        return {"dp": lax.rem(y + j, 4) * 2 + core}

    sibling = {"dp": y * 2 + 1 - core}

    barrier = pltpu.get_barrier_semaphore()
    peers = [along(a, j) for a in range(2) for j in (1, 2, 3)] + [along_y(1), along_y(3), sibling]
    for peer in peers:
        pl.semaphore_signal(barrier, inc=1, device_id=peer, device_id_type=MESH)

    inputs = [
        pltpu.make_async_copy(src, dst, in_sem.at[i])
        for i, (src, dst) in enumerate(
            (
                (tok_hbm, tok_ref), (gain_hbm, gain_ref), (shift_hbm, shift_ref),
                (bq_hbm, bq_ref), (bo_hbm, bo_ref),
            )
        )
    ]
    for copy in inputs:
        copy.start()

    w_copies = [
        pltpu.make_async_copy(w_hbm.at[c], w.at[:, pl.ds(c * F, F)], w_sem) for c in range(3)
    ]
    for copy in w_copies:
        copy.start()
    pl.semaphore_wait(barrier, len(peers))

    def remote(src, dst, send_sem, recv_sem, device):
        return pltpu.make_async_remote_copy(
            src_ref=src, dst_ref=dst, send_sem=send_sem, recv_sem=recv_sem,
            device_id=device, device_id_type=MESH,
        )

    piece = pl.ds(pl.multiple_of((core * 4 + y) * PR, PR), PR)

    def g1_copy(axis, j):
        return remote(
            wo_hbm.at[piece, pl.ds(axis * HC, HC)], g_hbm.at[axis, 3 - j, piece],
            g_send.at[0], g1_recv.at[axis, j // 2], along(axis, j),
        )

    def g2_copy(axis, j):
        k = 4 - j
        cols = pl.ds(0 if j == 1 else HC // 2, HC // 2)
        return remote(
            g_hbm.at[axis, k - 1, piece, cols], g_hbm.at[axis, 1, piece, cols],
            g_send.at[1], g2_recv.at[axis, j // 2], along(axis, j),
        )

    for axis in range(2):
        for j in (1, 3):
            g1_copy(axis, j).start()

    def norm_rows(i, carry):
        rows = pl.ds(pl.multiple_of(i * 16, 16), 16)
        v = tok_ref[rows, :].astype(jnp.float32)
        center = jnp.mean(v, axis=-1, keepdims=True)
        v = v - center
        spread = jnp.mean(v * v, axis=-1, keepdims=True)
        v = (v * lax.rsqrt(spread + EPS) * gain_ref[...] + shift_ref[...]).astype(jnp.bfloat16)
        for r in range(RINGS):
            for c in range(SUBS):
                ag[r, c, rows, :] = v[:, r * QW + c * CW : r * QW + (c + 1) * CW]
        return carry

    for copy in inputs:
        copy.wait()
    lax.fori_loop(0, ROWS // 16, norm_rows, 0)

    def slot(s):
        if isinstance(s, int):
            return pl.ds(s * ROWS, ROWS)
        return pl.ds(pl.multiple_of(s * ROWS, 16), ROWS)

    def ag_copy(r, c, s):
        return remote(
            ag.at[r, c, slot(s)], ag.at[r, c, slot(s + 1)],
            ag_send.at[r, c], ag_recv.at[r, c, lax.rem(s + 1, SPAN)], {"tp": nxt[r]},
        )

    def ag_arrived(r, c, s):
        return remote(
            ag.at[r, c, slot(s)], ag.at[r, c, slot(s)],
            ag_send.at[r, c], ag_recv.at[r, c, lax.rem(s, SPAN)], {"tp": nxt[r]},
        )

    for r in range(RINGS):
        ag_copy(r, 0, 0).start()
    for j in (1, 3):
        for axis in range(2):
            g1_copy(axis, j).wait_recv()
            g2_copy(axis, j).start()
    for c in range(1, SUBS):
        for r in range(RINGS):
            ag_copy(r, c, 0).start()

    for c in range(3):
        acc[:, c * F : (c + 1) * F] = jnp.broadcast_to(bq_ref[c : c + 1, :], (LEN, F))
    pltpu.make_async_copy(w, w, w_sem).wait()

    def gy_copy(axis, k, j):
        return remote(
            g_hbm.at[axis, k - 1, piece], g_hbm.at[axis, k - 1, piece],
            g_send.at[2 + axis], gy_recv.at[axis, k - 1, j // 2], along_y(j),
        )

    def gf_copy(axis, k):
        j = 1 if axis == 0 else 3
        src = pl.ds(pl.multiple_of((core * 4 + lax.rem(y + 4 - j, 4)) * PR, PR), PR)
        return remote(
            g_hbm.at[axis, k - 1, src], g_hbm.at[axis, k - 1, src],
            g_send.at[4], gf_recv.at[axis, k - 1], along_y(j),
        )

    for k in (1, 3, 2):
        if k == 2:
            for axis in range(2):
                for j in (1, 3):
                    g2_copy(axis, j).wait_recv()
        for axis in range(2):
            gy_copy(axis, k, 1 if axis == 0 else 3).start()
    for k in (1, 3, 2):
        for axis in range(2):
            gy_copy(axis, k, 3 if axis == 0 else 1).start()

    def unit(first, count, r, subs, cols):
        home = jnp.where(r < 2, 4 * z, 4 * x) + lax.rem(z + x, 4)
        rows = pl.ds(pl.multiple_of(first * ROWS, 16), count * ROWS)
        for lo, hi in cols:
            res = None
            for c in subs:
                wrow = pl.ds(pl.multiple_of(r * QW + c * CW, CW), CW)
                part = jnp.dot(ag[r, c, rows, :], w[wrow, lo:hi], preferred_element_type=jnp.float32)
                res = part if res is None else res + part
            for i in range(count):
                src = ring_tp(r, behind(r, home, first + i))
                to = pl.ds(pl.multiple_of(src * ROWS, 16), ROWS)
                acc[to, lo:hi] += res[i * ROWS : (i + 1) * ROWS]

    halves, whole = ((0, 640), (640, 1152)), ((0, 1152),)

    mine = pl.ds(pl.multiple_of(core * (4 * PR), 4 * PR), 4 * PR)

    def gd_copy(axis, k):
        return remote(
            g_hbm.at[axis, k - 1, mine], g_hbm.at[axis, k - 1, mine],
            g_send.at[5], gd_recv.at[axis, k - 1], sibling,
        )

    blocks = [(axis, k) for axis in range(2) for k in (1, 2, 3)]

    def ag_step(s, carry):
        first = jnp.where(s < 12, s - 4, 2 * s - 16)
        count = jnp.where(s < 4, 0, jnp.where(s < 12, 1, jnp.where(s < 14, 2, 0)))
        for c in range(SUBS):
            for r in range(RINGS):
                ag_arrived(r, c, s).wait_recv()
                ag_copy(r, c, s - 1).wait_send()
                ag_copy(r, c, s).start()

            def four(u, carry, c=c):
                unit(lax.div(u, RINGS) * 4, 4, lax.rem(u, RINGS), (c,), halves)
                return carry

            lax.fori_loop(first, first + count, four, 0)

        for i, k in enumerate((1, 3, 2)):

            @pl.when(s == FORWARD_AT + i)
            def _():
                for axis in range(2):
                    gy_copy(axis, k, 1 if axis == 0 else 3).wait_recv()
                    gf_copy(axis, k).start()

        @pl.when(s == 13)
        def _():
            for axis, k in blocks:
                gy_copy(axis, k, 3 if axis == 0 else 1).wait_recv()
                gf_copy(axis, k).wait_recv()
                gd_copy(axis, k).start()

        return carry

    lax.fori_loop(1, N - 1, ag_step, 0)

    def two(first):
        def step(r, carry):
            unit(first, 2, r, (0, 1, 2), whole)
            return carry

        lax.fori_loop(0, RINGS, step, 0)

    two(12)
    for c in range(SUBS):
        for r in range(RINGS):
            ag_arrived(r, c, N - 1).wait_recv()
            ag_copy(r, c, N - 2).wait_send()
    two(14)

    def to_bf16(i, carry):
        rows = pl.ds(pl.multiple_of(i * 64, 64), 64)
        qkv[rows, :] = acc[rows, :].astype(jnp.bfloat16)
        return carry

    lax.fori_loop(0, LEN // 64, to_bf16, 0)

    kv_copy = pltpu.make_async_copy(qkv.at[:, pl.ds(F, 2 * F)], kv_hbm, kv_sem)
    kv_copy.start()

    def home_of(n):
        if n < 8:
            return w, (n // 2) * KX, (n % 2) * CW
        return wx, 0, (n - 8) * CW

    def load(n, k):
        axis, m = n % 2, n // 2
        ref, row, col = home_of(n)
        if k == 0:
            src = wo_hbm.at[:, pl.ds(axis * HC + m * CW, CW)]
        else:
            src = g_hbm.at[axis, k - 1, :, pl.ds(m * CW, CW)]
        return pltpu.make_async_copy(src, ref.at[pl.ds(row + k * F, F), pl.ds(col, CW)], l_sem.at[n])

    def loaded(n):
        ref, row, col = home_of(n)
        chunk = ref.at[pl.ds(row, KX), pl.ds(col, CW)]
        return pltpu.make_async_copy(chunk, chunk, l_sem.at[n])

    last = len_ref[0] - 1

    def az_copy(h, j):
        src = att.at[pl.ds(pl.multiple_of(lax.rem(z + j, 4) * BQ, 64), BQ), pl.ds(h * HD, HD)]
        there = pl.ds((4 - j) * F + h * HD, HD)
        return remote(src, gat.at[1, :, there], az_send.at[h], az_recv.at[h, 3 - j], along(1, j))

    def ax_copy(h, qi, j):
        block = pl.ds(pl.multiple_of((4 * qi + lax.rem(x + j, 4)) * ROWS, 16), ROWS)
        src = att.at[block, pl.ds(h * HD, HD)]
        there = pl.ds((4 - j) * F + h * HD, HD)
        return remote(
            src, gat.at[0, pl.ds(qi * ROWS, ROWS), there], ax_send.at[h], ax_recv.at[h, 3 - j], along(0, j)
        )

    def a_all(axis, h, k):
        part = gat.at[axis, :, pl.ds(h * HD, HD)]
        sends, recvs = ((ax_send, ax_recv), (az_send, az_recv))[axis]
        return remote(part, part, sends.at[h], recvs.at[h, k - 1], along(axis, k))

    def a_sent(axis, h):
        part = gat.at[axis, :, pl.ds(0, 3 * HD)]
        return remote(part, part, (ax_send, az_send)[axis].at[h], ax_recv.at[h, 0], along(0, 1))

    for h in range(HEADS):
        q0, k0, v0 = h * HD, F + h * HD, 2 * F + h * HD
        for row in range(0, LEN, QB):
            kv = row + QB
            free = min(row, LEN // 2)
            q = qkv[row:kv, q0 : q0 + HD]
            k = qkv[0:kv, k0 : k0 + HD]
            v = qkv[0:kv, v0 : v0 + HD]
            sc = lax.dot_general(q, k, (((1,), (1,)), ((), ())), preferred_element_type=jnp.float32)
            limit = jnp.minimum(lax.broadcasted_iota(jnp.int32, (QB, 1), 0) + row, last)
            key = lax.broadcasted_iota(jnp.int32, (QB, kv - free), 1) + free
            masked = jnp.where(key <= limit, sc[:, free:], -1e30)
            sc = jnp.concatenate([sc[:, :free], masked], axis=1) if free else masked
            top = jnp.max(sc, axis=-1, keepdims=True)
            e = jnp.exp2((sc - top) * SCALE2)
            inv = 1.0 / jnp.sum(e, axis=-1, keepdims=True)
            p = (e * inv).astype(jnp.bfloat16)
            o = jnp.dot(p, v, preferred_element_type=jnp.float32)
            att[row:kv, q0 : q0 + HD] = o.astype(jnp.bfloat16)
            for qi in range(4):
                if row < (qi + 1) * BQ <= kv:
                    for j in (2, 1, 3):
                        ax_copy(h, qi, j).start()
        for j in (2, 1, 3):
            az_copy(h, j).start()
        if h == 0:
            for axis, k in blocks:
                gd_copy(axis, k).wait_recv()
            for n in range(CHUNKS):
                for k in range(4):
                    load(n, k).start()

    for b in range(4):
        gat[0, b * ROWS : (b + 1) * ROWS, 0:F] = att[pl.ds(pl.multiple_of((4 * b + x) * ROWS, 16), ROWS), :]
    gat[1, :, 0:F] = att[pl.ds(pl.multiple_of(z * BQ, 64), BQ), :]

    def out_copy(n):
        lo = (n % 2) * HC + (n // 2) * CW
        return pltpu.make_async_copy(out.at[n], out_ref.at[:, pl.ds(lo, CW)], out_sem.at[n])

    def p_copy(n, what):
        axis, ahead = 1 - n % 2, (1 if (n // 2) % 2 == 0 else 3)
        here = x if axis == 0 else z
        j = (ahead, ahead, 4 - ahead)[what]
        block = lax.rem(here + (2 if what == 0 else j), 4)
        return remote(
            psend.at[n, block], prec.at[n, what], p_send.at[n],
            p0_recv.at[n] if what == 0 else p_recv.at[n], along(axis, j),
        )

    def p_all(n, count):
        part = prec.at[n, pl.ds(0, count)]
        return remote(part, part, p_send.at[n], p_recv.at[n], along(0, 1))

    def p_add(n):
        axis, ahead = 1 - n % 2, (1 if (n // 2) % 2 == 0 else 3)
        block = lax.rem((x if axis == 0 else z) + ahead, 4)
        p_copy(n, 0).wait_recv()
        both = psend[n, block].astype(jnp.float32) + prec[n, 0].astype(jnp.float32)
        psend[n, block] = both.astype(jnp.bfloat16)
        p_copy(n, 1).start()

    for n in range(CHUNKS):
        ref, row, col = home_of(n)
        if n < 2:
            for h in range(HEADS):
                for k in (1, 2, 3):
                    a_all(n, h, k).wait_recv()
        loaded(n).wait()
        res = jnp.dot(gat[n % 2], ref[row : row + KX, col : col + CW], preferred_element_type=jnp.float32)
        psend[n] = res.astype(jnp.bfloat16).reshape(4, ROWS, CW)
        p_copy(n, 0).start()
        p_copy(n, 2).start()
        if n >= LAG:
            p_add(n - LAG)
    for n in range(CHUNKS - LAG, CHUNKS):
        p_add(n)

    for n in range(CHUNKS):
        here = z if n % 2 == 0 else x
        lo = (n % 2) * HC + (n // 2) * CW
        total = psend[n, here].astype(jnp.float32) + bo_ref[:, lo : lo + CW]
        p_all(n, 2).wait_recv()
        total += prec[n, 1].astype(jnp.float32) + prec[n, 2].astype(jnp.float32)
        out[n] = total.astype(jnp.bfloat16)
        out_copy(n).start()

    for n in range(CHUNKS):
        p_all(n, 3).wait_send()
    for i, sent in enumerate(
        (
            g_hbm.at[0, 0, pl.ds(0, 4 * PR)],
            g_hbm.at[0, 0, pl.ds(0, 2 * PR)],
            g_hbm.at[0, 0, pl.ds(0, 6 * PR)],
            g_hbm.at[0, 0, pl.ds(0, 6 * PR)],
            g_hbm.at[0, 0, pl.ds(0, 6 * PR)],
            g_hbm.at[0],
        )
    ):
        remote(sent, sent, g_send.at[i], gd_recv.at[0, 0], sibling).wait_send()
    for h in range(HEADS):
        for axis in range(2):
            a_sent(axis, h).wait_send()
    for n in range(CHUNKS):
        out_copy(n).wait()
    kv_copy.wait()


def finish_kernel(page_ref, len_ref, part_hbm, new_hbm, old_hbm, out_hbm, kv_hbm, part, new, kv, in_sem, out_sem):
    group = SLOTS * PAGE // 4
    news = [
        pltpu.make_async_copy(new_hbm.at[pl.ds(g * BQ, BQ)], new.at[pl.ds(g * BQ, BQ)], in_sem.at[g])
        for g in range(4)
    ]
    olds = [
        pltpu.make_async_copy(
            old_hbm.at[:, pl.ds(g * group, group)], kv.at[:, pl.ds(g * group, group)], in_sem.at[4 + g]
        )
        for g in range(4)
    ]
    kvs = [
        pltpu.make_async_copy(
            kv.at[:, pl.ds(g * group, group)], kv_hbm.at[:, pl.ds(g * group, group)], out_sem.at[g]
        )
        for g in range(4)
    ]
    load = pltpu.make_async_copy(part_hbm, part, in_sem.at[8])
    store = pltpu.make_async_copy(part, out_hbm, out_sem.at[4])
    for copy in [*news, *olds, load]:
        copy.start()
    for copy in news:
        copy.wait()
    for g in range(4):
        olds[g].wait()
        for i in range(g * SLOTS // 4, (g + 1) * SLOTS // 4):
            page = jnp.int32(-1)
            for p in range(PAGES):
                page = jnp.where(page_ref[0, p] == i, p, page)
            row = lax.broadcasted_iota(jnp.int32, (PAGE, 1), 0) + page * PAGE
            written = (row < len_ref[0]) & (row >= 0)
            rows = pl.ds(pl.multiple_of(jnp.maximum(page, 0) * PAGE, PAGE), PAGE)
            for c in range(2):
                old = kv[c, i * PAGE : (i + 1) * PAGE, :]
                kv[c, i * PAGE : (i + 1) * PAGE, :] = jnp.where(written, new[rows, c * F : (c + 1) * F], old)
        kvs[g].start()
    load.wait()
    store.start()
    for copy in [*kvs, store]:
        copy.wait()


def body(tokens, ln_gain, ln_bias, w_qkv, b_qkv, w_out, b_out, kv_cache, page_table, lengths):
    anym = pl.BlockSpec(memory_space=pl.ANY)
    smem = pl.BlockSpec(memory_space=pltpu.SMEM)
    dma = pltpu.SemaphoreType.DMA
    part, kv_new, _ = pl.pallas_call(
        main_kernel,
        out_shape=(
            jax.ShapeDtypeStruct((ROWS, D), jnp.bfloat16),
            jax.ShapeDtypeStruct((LEN, 2 * F), jnp.bfloat16),
            jax.ShapeDtypeStruct((2, 3, F, HC), jnp.bfloat16),
        ),
        in_specs=[smem] + [anym] * 7,
        out_specs=(anym, anym, anym),
        scratch_shapes=[
            pltpu.VMEM((RINGS, SUBS, LEN, CW), jnp.bfloat16),
            pltpu.VMEM((D, 3 * F), jnp.bfloat16),
            pltpu.VMEM((LEN, 3 * F), jnp.float32),
            pltpu.VMEM((LEN, 3 * F), jnp.bfloat16),
            pltpu.VMEM((LEN, F), jnp.bfloat16),
            pltpu.VMEM((KX, 4 * CW), jnp.bfloat16),
            pltpu.VMEM((2, BQ, KX), jnp.bfloat16),
            pltpu.VMEM((CHUNKS, 4, ROWS, CW), jnp.bfloat16),
            pltpu.VMEM((CHUNKS, 3, ROWS, CW), jnp.bfloat16),
            pltpu.VMEM((CHUNKS, ROWS, CW), jnp.bfloat16),
            pltpu.VMEM((ROWS, D), jnp.bfloat16),
            pltpu.VMEM((1, D), jnp.float32),
            pltpu.VMEM((1, D), jnp.float32),
            pltpu.VMEM((3, F), jnp.float32),
            pltpu.VMEM((1, D), jnp.float32),
            dma((5,)),
            dma((RINGS, SUBS)),
            dma((RINGS, SUBS, SPAN)),
            dma,
            dma,
            dma((CHUNKS,)),
            dma((6,)),
            dma((2, 2)),
            dma((2, 2)),
            dma((2, 3, 2)),
            dma((2, 3)),
            dma((2, 3)),
            dma((CHUNKS,)),
            dma((HEADS,)),
            dma((HEADS, 3)),
            dma((HEADS,)),
            dma((HEADS, 3)),
            dma((CHUNKS,)),
            dma((CHUNKS,)),
            dma((CHUNKS,)),
        ],
        compiler_params=pltpu.CompilerParams(
            collective_id=0, has_side_effects=True, vmem_limit_bytes=67043328
        ),
        name="sublayer",
    )(
        lengths,
        tokens,
        ln_gain.reshape(1, D),
        ln_bias.reshape(1, D),
        jnp.transpose(w_qkv, (1, 0, 2)),
        b_qkv,
        w_out,
        b_out.reshape(1, D),
    )
    out, kv_out = pl.pallas_call(
        finish_kernel,
        out_shape=(
            jax.ShapeDtypeStruct((ROWS, D), jnp.bfloat16),
            jax.ShapeDtypeStruct((2, SLOTS * PAGE, F), jnp.bfloat16),
        ),
        in_specs=[smem, smem, anym, anym, anym],
        out_specs=(anym, anym),
        scratch_shapes=[
            pltpu.VMEM((ROWS, D), jnp.bfloat16),
            pltpu.VMEM((LEN, 2 * F), jnp.bfloat16),
            pltpu.VMEM((2, SLOTS * PAGE, F), jnp.bfloat16),
            dma((9,)),
            dma((5,)),
        ],
        name="finish",
    )(page_table, lengths, part, kv_new, kv_cache.reshape(2, SLOTS * PAGE, F))
    return out, kv_out.reshape(kv_cache.shape)


def solution(mesh):
    placed = (
        P(("dp", "tp"), None),
        P(),
        P(),
        P(None, None, "tp"),
        P(None, "tp"),
        P("tp", None),
        P(),
        P(None, "dp", None, "tp"),
        P("dp", None),
        P("dp"),
    )
    return jax.shard_map(
        body,
        mesh=mesh,
        in_specs=placed,
        out_specs=(P(("dp", "tp"), None), P(None, "dp", None, "tp")),
        check_vma=False,
    )
```

```python
import functools

import jax
import jax.numpy as jnp
from jax import lax
from jax.experimental import pallas as pl
from jax.experimental.pallas import tpu as pltpu
from jax.sharding import PartitionSpec as P

HD = 128
EPS = 1e-05
MESH = pl.DeviceIdType.MESH
RINGS = 4
SUBS = 3
N = 16
ROWS = 80
CW = 512
QW = SUBS * CW
D = RINGS * QW
LEN = N * ROWS
F = 384
HEADS = F // HD
BQ = 320
BATCH = 4
PAGE = 128
PAGES = LEN // PAGE
SLOTS = 12
HC = D // 2
PR = F // 8
KX = 4 * F
CHUNKS = 12
LAG = 4
QB = 256
PIECES = ((0, 320, 0), (320, 640, 1), (640, 960, 2), (960, 1024, 3), (1024, 1280, 3))
SPAN = 4
FORWARD_AT = 4
SCALE2 = 1.4426950408889634 / (HD ** 0.5)


def ring_tp(ring, pos):
    a = lax.div(pos, 4)
    b = lax.rem(lax.rem(pos, 4) - a + 4, 4)
    return jnp.where(ring < 2, a * 4 + b, b * 4 + a)


def my_pos(ring, z, x):
    t = lax.rem(z + x, 4)
    return jnp.where(ring < 2, 4 * z + t, 4 * x + t)


def behind(ring, pos, k):
    up = lax.rem(ring, 2)
    return lax.rem(jnp.where(up == 0, pos + N - k, pos + k), N)


def main_kernel(
    len_ref, tok_hbm, gain_hbm, shift_hbm, w_hbm, bq_hbm, wo_hbm, bo_hbm,
    out_ref, kv_hbm, g_hbm,
    ag, w, acc, qkv, att, wx, gat, psend, prec, out,
    tok_ref, gain_ref, shift_ref, bq_ref, bo_ref, in_sem,
    ag_send, ag_recv, w_sem, kv_sem, out_sem,
    g_send, g1_recv, g2_recv, gy_recv, gf_recv, gd_recv,
    l_sem, az_send, az_recv, ax_send, ax_recv, p_send, p0_recv, p_recv,
):
    tp = lax.axis_index("tp")
    dp = lax.axis_index("dp")
    z = lax.div(tp, 4)
    x = lax.rem(tp, 4)
    y = lax.div(dp, 2)
    core = lax.rem(dp, 2)
    pos = [my_pos(jnp.int32(r), z, x) for r in range(RINGS)]
    nxt = [ring_tp(jnp.int32(r), behind(jnp.int32(r), pos[r], N - 1)) for r in range(RINGS)]

    def along(axis, j):
        if axis == 0:
            return {"tp": z * 4 + lax.rem(x + j, 4)}
        return {"tp": lax.rem(z + j, 4) * 4 + x}

    def along_y(j):
        return {"dp": lax.rem(y + j, 4) * 2 + core}

    sibling = {"dp": y * 2 + 1 - core}

    barrier = pltpu.get_barrier_semaphore()
    peers = [along(a, j) for a in range(2) for j in (1, 2, 3)] + [along_y(1), along_y(3), sibling]
    for peer in peers:
        pl.semaphore_signal(barrier, inc=1, device_id=peer, device_id_type=MESH)

    inputs = [
        pltpu.make_async_copy(src, dst, in_sem.at[i])
        for i, (src, dst) in enumerate(
            (
                (tok_hbm, tok_ref), (gain_hbm, gain_ref), (shift_hbm, shift_ref),
                (bq_hbm, bq_ref), (bo_hbm, bo_ref),
            )
        )
    ]
    for copy in inputs:
        copy.start()

    w_copies = [
        pltpu.make_async_copy(w_hbm.at[c], w.at[:, pl.ds(c * F, F)], w_sem) for c in range(3)
    ]
    for copy in w_copies:
        copy.start()
    pl.semaphore_wait(barrier, len(peers))

    def remote(src, dst, send_sem, recv_sem, device):
        return pltpu.make_async_remote_copy(
            src_ref=src, dst_ref=dst, send_sem=send_sem, recv_sem=recv_sem,
            device_id=device, device_id_type=MESH,
        )

    piece = pl.ds(pl.multiple_of((core * 4 + y) * PR, PR), PR)

    def g1_copy(axis, j):
        return remote(
            wo_hbm.at[piece, pl.ds(axis * HC, HC)], g_hbm.at[axis, 3 - j, piece],
            g_send.at[0], g1_recv.at[axis, j // 2], along(axis, j),
        )

    def g2_copy(axis, j):
        k = 4 - j
        cols = pl.ds(0 if j == 1 else HC // 2, HC // 2)
        return remote(
            g_hbm.at[axis, k - 1, piece, cols], g_hbm.at[axis, 1, piece, cols],
            g_send.at[1], g2_recv.at[axis, j // 2], along(axis, j),
        )

    for axis in range(2):
        for j in (1, 3):
            g1_copy(axis, j).start()

    def norm_rows(i, carry):
        rows = pl.ds(pl.multiple_of(i * 16, 16), 16)
        v = tok_ref[rows, :].astype(jnp.float32)
        center = jnp.mean(v, axis=-1, keepdims=True)
        v = v - center
        spread = jnp.mean(v * v, axis=-1, keepdims=True)
        v = (v * lax.rsqrt(spread + EPS) * gain_ref[...] + shift_ref[...]).astype(jnp.bfloat16)
        for r in range(RINGS):
            for c in range(SUBS):
                ag[r, c, rows, :] = v[:, r * QW + c * CW : r * QW + (c + 1) * CW]
        return carry

    for copy in inputs:
        copy.wait()
    lax.fori_loop(0, ROWS // 16, norm_rows, 0)

    def slot(s):
        if isinstance(s, int):
            return pl.ds(s * ROWS, ROWS)
        return pl.ds(pl.multiple_of(s * ROWS, 16), ROWS)

    def ag_copy(r, c, s):
        return remote(
            ag.at[r, c, slot(s)], ag.at[r, c, slot(s + 1)],
            ag_send.at[r, c], ag_recv.at[r, c, lax.rem(s + 1, SPAN)], {"tp": nxt[r]},
        )

    def ag_arrived(r, c, s):
        return remote(
            ag.at[r, c, slot(s)], ag.at[r, c, slot(s)],
            ag_send.at[r, c], ag_recv.at[r, c, lax.rem(s, SPAN)], {"tp": nxt[r]},
        )

    for r in range(RINGS):
        ag_copy(r, 0, 0).start()
    for j in (1, 3):
        for axis in range(2):
            g1_copy(axis, j).wait_recv()
            g2_copy(axis, j).start()
    for c in range(1, SUBS):
        for r in range(RINGS):
            ag_copy(r, c, 0).start()

    for c in range(3):
        acc[:, c * F : (c + 1) * F] = jnp.broadcast_to(bq_ref[c : c + 1, :], (LEN, F))
    pltpu.make_async_copy(w, w, w_sem).wait()

    def gy_copy(axis, k, j):
        return remote(
            g_hbm.at[axis, k - 1, piece], g_hbm.at[axis, k - 1, piece],
            g_send.at[2 + axis], gy_recv.at[axis, k - 1, j // 2], along_y(j),
        )

    def gf_copy(axis, k):
        j = 1 if axis == 0 else 3
        src = pl.ds(pl.multiple_of((core * 4 + lax.rem(y + 4 - j, 4)) * PR, PR), PR)
        return remote(
            g_hbm.at[axis, k - 1, src], g_hbm.at[axis, k - 1, src],
            g_send.at[4], gf_recv.at[axis, k - 1], along_y(j),
        )

    for k in (1, 3, 2):
        if k == 2:
            for axis in range(2):
                for j in (1, 3):
                    g2_copy(axis, j).wait_recv()
        for axis in range(2):
            gy_copy(axis, k, 1 if axis == 0 else 3).start()
    for k in (1, 3, 2):
        for axis in range(2):
            gy_copy(axis, k, 3 if axis == 0 else 1).start()

    def unit(first, count, r, subs, cols):
        home = jnp.where(r < 2, 4 * z, 4 * x) + lax.rem(z + x, 4)
        rows = pl.ds(pl.multiple_of(first * ROWS, 16), count * ROWS)
        for lo, hi in cols:
            res = None
            for c in subs:
                wrow = pl.ds(pl.multiple_of(r * QW + c * CW, CW), CW)
                part = jnp.dot(ag[r, c, rows, :], w[wrow, lo:hi], preferred_element_type=jnp.float32)
                res = part if res is None else res + part
            for i in range(count):
                src = ring_tp(r, behind(r, home, first + i))
                to = pl.ds(pl.multiple_of(src * ROWS, 16), ROWS)
                acc[to, lo:hi] += res[i * ROWS : (i + 1) * ROWS]

    halves, whole = ((0, 640), (640, 1152)), ((0, 1152),)

    mine = pl.ds(pl.multiple_of(core * (4 * PR), 4 * PR), 4 * PR)

    def gd_copy(axis, k):
        return remote(
            g_hbm.at[axis, k - 1, mine], g_hbm.at[axis, k - 1, mine],
            g_send.at[5], gd_recv.at[axis, k - 1], sibling,
        )

    blocks = [(axis, k) for axis in range(2) for k in (1, 2, 3)]

    def ag_step(s, carry):
        first = jnp.where(s < 12, s - 4, 2 * s - 16)
        count = jnp.where(s < 4, 0, jnp.where(s < 12, 1, jnp.where(s < 14, 2, 0)))
        for c in range(SUBS):
            for r in range(RINGS):
                ag_arrived(r, c, s).wait_recv()
                ag_copy(r, c, s - 1).wait_send()
                ag_copy(r, c, s).start()

            def four(u, carry, c=c):
                unit(lax.div(u, RINGS) * 4, 4, lax.rem(u, RINGS), (c,), halves)
                return carry

            lax.fori_loop(first, first + count, four, 0)

        for i, k in enumerate((1, 3, 2)):

            @pl.when(s == FORWARD_AT + i)
            def _():
                for axis in range(2):
                    gy_copy(axis, k, 1 if axis == 0 else 3).wait_recv()
                    gf_copy(axis, k).start()

        @pl.when(s == 13)
        def _():
            for axis, k in blocks:
                gy_copy(axis, k, 3 if axis == 0 else 1).wait_recv()
                gf_copy(axis, k).wait_recv()
                gd_copy(axis, k).start()

        return carry

    lax.fori_loop(1, N - 1, ag_step, 0)

    def two(first):
        def step(r, carry):
            unit(first, 2, r, (0, 1, 2), whole)
            return carry

        lax.fori_loop(0, RINGS, step, 0)

    two(12)
    for c in range(SUBS):
        for r in range(RINGS):
            ag_arrived(r, c, N - 1).wait_recv()
            ag_copy(r, c, N - 2).wait_send()
    two(14)

    def to_bf16(i, carry):
        rows = pl.ds(pl.multiple_of(i * 64, 64), 64)
        qkv[rows, :] = acc[rows, :].astype(jnp.bfloat16)
        return carry

    lax.fori_loop(0, LEN // 64, to_bf16, 0)

    kv_copy = pltpu.make_async_copy(qkv.at[:, pl.ds(F, 2 * F)], kv_hbm, kv_sem)
    kv_copy.start()

    def home_of(n):
        if n < 8:
            return w, (n // 2) * KX, (n % 2) * CW
        return wx, 0, (n - 8) * CW

    def load(n, k):
        axis, m = n % 2, n // 2
        ref, row, col = home_of(n)
        if k == 0:
            src = wo_hbm.at[:, pl.ds(axis * HC + m * CW, CW)]
        else:
            src = g_hbm.at[axis, k - 1, :, pl.ds(m * CW, CW)]
        return pltpu.make_async_copy(src, ref.at[pl.ds(row + k * F, F), pl.ds(col, CW)], l_sem.at[n])

    def loaded(n):
        ref, row, col = home_of(n)
        chunk = ref.at[pl.ds(row, KX), pl.ds(col, CW)]
        return pltpu.make_async_copy(chunk, chunk, l_sem.at[n])

    last = len_ref[0] - 1

    def az_copy(h, lo, hi, qi, k):
        src = att.at[pl.ds(lo, hi - lo), pl.ds(h * HD, HD)]
        there = pl.ds(pl.multiple_of(k * F + h * HD, HD), HD)
        return remote(
            src, gat.at[1, pl.ds(lo - qi * BQ, hi - lo), there],
            az_send.at[h], az_recv.at[h, k - 1], {"tp": qi * 4 + x},
        )

    def ax_copy(h, qi, j):
        block = pl.ds(pl.multiple_of((4 * qi + lax.rem(x + j, 4)) * ROWS, 16), ROWS)
        src = att.at[block, pl.ds(h * HD, HD)]
        there = pl.ds((4 - j) * F + h * HD, HD)
        return remote(
            src, gat.at[0, pl.ds(qi * ROWS, ROWS), there], ax_send.at[h], ax_recv.at[h, 3 - j], along(0, j)
        )

    def a_all(axis, h, k):
        part = gat.at[axis, :, pl.ds(h * HD, HD)]
        sends, recvs = ((ax_send, ax_recv), (az_send, az_recv))[axis]
        return remote(part, part, sends.at[h], recvs.at[h, k - 1], along(axis, k))

    def a_sent(axis, h):
        part = gat.at[axis, :, pl.ds(0, 3 * HD)]
        return remote(part, part, (ax_send, az_send)[axis].at[h], ax_recv.at[h, 0], along(0, 1))

    for h in range(HEADS):
        q0, k0, v0 = h * HD, F + h * HD, 2 * F + h * HD
        for row in range(0, LEN, QB):
            kv = row + QB
            free = min(row, LEN // 2)
            q = qkv[row:kv, q0 : q0 + HD]
            k = qkv[0:kv, k0 : k0 + HD]
            v = qkv[0:kv, v0 : v0 + HD]
            sc = lax.dot_general(q, k, (((1,), (1,)), ((), ())), preferred_element_type=jnp.float32)
            limit = jnp.minimum(lax.broadcasted_iota(jnp.int32, (QB, 1), 0) + row, last)
            key = lax.broadcasted_iota(jnp.int32, (QB, kv - free), 1) + free
            masked = jnp.where(key <= limit, sc[:, free:], -1e30)
            sc = jnp.concatenate([sc[:, :free], masked], axis=1) if free else masked
            top = jnp.max(sc, axis=-1, keepdims=True)
            e = jnp.exp2((sc - top) * SCALE2)
            inv = 1.0 / jnp.sum(e, axis=-1, keepdims=True)
            p = (e * inv).astype(jnp.bfloat16)
            o = jnp.dot(p, v, preferred_element_type=jnp.float32)
            att[row:kv, q0 : q0 + HD] = o.astype(jnp.bfloat16)
            for lo, hi, qi in PIECES:
                if row < hi <= kv:

                    @pl.when(z != qi)
                    def _():
                        az_copy(h, lo, hi, qi, lax.rem(z - qi + 4, 4)).start()

                    if hi == (qi + 1) * BQ:
                        for j in (2, 1, 3):
                            ax_copy(h, qi, j).start()
        if h == 0:
            for axis, k in blocks:
                gd_copy(axis, k).wait_recv()
            for n in range(CHUNKS):
                for k in range(4):
                    load(n, k).start()

    for b in range(4):
        gat[0, b * ROWS : (b + 1) * ROWS, 0:F] = att[pl.ds(pl.multiple_of((4 * b + x) * ROWS, 16), ROWS), :]
    gat[1, :, 0:F] = att[pl.ds(pl.multiple_of(z * BQ, 64), BQ), :]

    def out_copy(n):
        lo = (n % 2) * HC + (n // 2) * CW
        return pltpu.make_async_copy(out.at[n], out_ref.at[:, pl.ds(lo, CW)], out_sem.at[n])

    def p_copy(n, what):
        axis, ahead = 1 - n % 2, (1 if (n // 2) % 2 == 0 else 3)
        here = x if axis == 0 else z
        j = (ahead, ahead, 4 - ahead)[what]
        block = lax.rem(here + (2 if what == 0 else j), 4)
        return remote(
            psend.at[n, block], prec.at[n, what], p_send.at[n],
            p0_recv.at[n] if what == 0 else p_recv.at[n], along(axis, j),
        )

    def p_all(n, count):
        part = prec.at[n, pl.ds(0, count)]
        return remote(part, part, p_send.at[n], p_recv.at[n], along(0, 1))

    def p_add(n):
        axis, ahead = 1 - n % 2, (1 if (n // 2) % 2 == 0 else 3)
        block = lax.rem((x if axis == 0 else z) + ahead, 4)
        p_copy(n, 0).wait_recv()
        both = psend[n, block].astype(jnp.float32) + prec[n, 0].astype(jnp.float32)
        psend[n, block] = both.astype(jnp.bfloat16)
        p_copy(n, 1).start()

    for n in range(CHUNKS):
        ref, row, col = home_of(n)
        if n < 2:
            for h in range(HEADS):
                for k in (1, 2, 3):
                    a_all(n, h, k).wait_recv()
        loaded(n).wait()
        res = jnp.dot(gat[n % 2], ref[row : row + KX, col : col + CW], preferred_element_type=jnp.float32)
        psend[n] = res.astype(jnp.bfloat16).reshape(4, ROWS, CW)
        p_copy(n, 0).start()
        p_copy(n, 2).start()
        if n >= LAG:
            p_add(n - LAG)
    for n in range(CHUNKS - LAG, CHUNKS):
        p_add(n)

    for n in range(CHUNKS):
        here = z if n % 2 == 0 else x
        lo = (n % 2) * HC + (n // 2) * CW
        total = psend[n, here].astype(jnp.float32) + bo_ref[:, lo : lo + CW]
        p_all(n, 2).wait_recv()
        total += prec[n, 1].astype(jnp.float32) + prec[n, 2].astype(jnp.float32)
        out[n] = total.astype(jnp.bfloat16)
        out_copy(n).start()

    for n in range(CHUNKS):
        p_all(n, 3).wait_send()
    for i, sent in enumerate(
        (
            g_hbm.at[0, 0, pl.ds(0, 4 * PR)],
            g_hbm.at[0, 0, pl.ds(0, 2 * PR)],
            g_hbm.at[0, 0, pl.ds(0, 6 * PR)],
            g_hbm.at[0, 0, pl.ds(0, 6 * PR)],
            g_hbm.at[0, 0, pl.ds(0, 6 * PR)],
            g_hbm.at[0],
        )
    ):
        remote(sent, sent, g_send.at[i], gd_recv.at[0, 0], sibling).wait_send()
    for h in range(HEADS):
        for axis in range(2):
            a_sent(axis, h).wait_send()
    for n in range(CHUNKS):
        out_copy(n).wait()
    kv_copy.wait()


def finish_kernel(page_ref, len_ref, part_hbm, new_hbm, old_hbm, out_hbm, kv_hbm, part, new, kv, in_sem, out_sem):
    load = pltpu.make_async_copy(part_hbm, part, in_sem.at[SLOTS])
    load.start()

    def rows_of(i):
        return pl.ds(pl.multiple_of(i * PAGE, PAGE), PAGE)

    def old_copy(i):
        return pltpu.make_async_copy(old_hbm.at[:, rows_of(i)], kv.at[:, rows_of(i)], in_sem.at[i])

    def kv_copy(i):
        return pltpu.make_async_copy(kv.at[:, rows_of(i)], kv_hbm.at[:, rows_of(i)], out_sem.at[i])

    def new_copy(page):
        return pltpu.make_async_copy(new_hbm.at[rows_of(page)], new, in_sem.at[SLOTS + 1])

    used = []
    for i in range(SLOTS):
        page = jnp.int32(-1)
        for p in range(PAGES):
            page = jnp.where(page_ref[0, p] == i, p, page)
        count = jnp.where(page < 0, 0, jnp.clip(len_ref[0] - page * PAGE, 0, PAGE))
        page = jnp.maximum(page, 0)
        used.append((page, count))

        @pl.when(count == PAGE)
        def _():
            for c in range(2):
                pltpu.make_async_copy(
                    new_hbm.at[rows_of(page), pl.ds(c * F, F)], kv.at[c, rows_of(i)], in_sem.at[i]
                ).start()

        @pl.when(count < PAGE)
        def _():
            old_copy(i).start()

        @pl.when((count > 0) & (count < PAGE))
        def _():
            new_copy(page).start()

    store = pltpu.make_async_copy(part, out_hbm, out_sem.at[SLOTS])
    load.wait()
    store.start()
    for i, (page, count) in enumerate(used):
        old_copy(i).wait()

        @pl.when((count > 0) & (count < PAGE))
        def _():
            new_copy(page).wait()
            written = lax.broadcasted_iota(jnp.int32, (PAGE, 1), 0) < count
            for c in range(2):
                rows = pl.ds(i * PAGE, PAGE)
                kv[c, rows, :] = jnp.where(written, new[:, c * F : (c + 1) * F], kv[c, rows, :])

        kv_copy(i).start()
    for i in range(SLOTS):
        kv_copy(i).wait()
    store.wait()


def body(tokens, ln_gain, ln_bias, w_qkv, b_qkv, w_out, b_out, kv_cache, page_table, lengths):
    anym = pl.BlockSpec(memory_space=pl.ANY)
    smem = pl.BlockSpec(memory_space=pltpu.SMEM)
    dma = pltpu.SemaphoreType.DMA
    part, kv_new, _ = pl.pallas_call(
        main_kernel,
        out_shape=(
            jax.ShapeDtypeStruct((ROWS, D), jnp.bfloat16),
            jax.ShapeDtypeStruct((LEN, 2 * F), jnp.bfloat16),
            jax.ShapeDtypeStruct((2, 3, F, HC), jnp.bfloat16),
        ),
        in_specs=[smem] + [anym] * 7,
        out_specs=(anym, anym, anym),
        scratch_shapes=[
            pltpu.VMEM((RINGS, SUBS, LEN, CW), jnp.bfloat16),
            pltpu.VMEM((D, 3 * F), jnp.bfloat16),
            pltpu.VMEM((LEN, 3 * F), jnp.float32),
            pltpu.VMEM((LEN, 3 * F), jnp.bfloat16),
            pltpu.VMEM((LEN, F), jnp.bfloat16),
            pltpu.VMEM((KX, 4 * CW), jnp.bfloat16),
            pltpu.VMEM((2, BQ, KX), jnp.bfloat16),
            pltpu.VMEM((CHUNKS, 4, ROWS, CW), jnp.bfloat16),
            pltpu.VMEM((CHUNKS, 3, ROWS, CW), jnp.bfloat16),
            pltpu.VMEM((CHUNKS, ROWS, CW), jnp.bfloat16),
            pltpu.VMEM((ROWS, D), jnp.bfloat16),
            pltpu.VMEM((1, D), jnp.float32),
            pltpu.VMEM((1, D), jnp.float32),
            pltpu.VMEM((3, F), jnp.float32),
            pltpu.VMEM((1, D), jnp.float32),
            dma((5,)),
            dma((RINGS, SUBS)),
            dma((RINGS, SUBS, SPAN)),
            dma,
            dma,
            dma((CHUNKS,)),
            dma((6,)),
            dma((2, 2)),
            dma((2, 2)),
            dma((2, 3, 2)),
            dma((2, 3)),
            dma((2, 3)),
            dma((CHUNKS,)),
            dma((HEADS,)),
            dma((HEADS, 3)),
            dma((HEADS,)),
            dma((HEADS, 3)),
            dma((CHUNKS,)),
            dma((CHUNKS,)),
            dma((CHUNKS,)),
        ],
        compiler_params=pltpu.CompilerParams(
            collective_id=0, has_side_effects=True, vmem_limit_bytes=67043328
        ),
        name="sublayer",
    )(
        lengths,
        tokens,
        ln_gain.reshape(1, D),
        ln_bias.reshape(1, D),
        jnp.transpose(w_qkv, (1, 0, 2)),
        b_qkv,
        w_out,
        b_out.reshape(1, D),
    )
    out, kv_out = pl.pallas_call(
        finish_kernel,
        out_shape=(
            jax.ShapeDtypeStruct((ROWS, D), jnp.bfloat16),
            jax.ShapeDtypeStruct((2, SLOTS * PAGE, F), jnp.bfloat16),
        ),
        in_specs=[smem, smem, anym, anym, anym],
        out_specs=(anym, anym),
        scratch_shapes=[
            pltpu.VMEM((ROWS, D), jnp.bfloat16),
            pltpu.VMEM((PAGE, 2 * F), jnp.bfloat16),
            pltpu.VMEM((2, SLOTS * PAGE, F), jnp.bfloat16),
            dma((SLOTS + 2,)),
            dma((SLOTS + 1,)),
        ],
        name="finish",
    )(page_table, lengths, part, kv_new, kv_cache.reshape(2, SLOTS * PAGE, F))
    return out, kv_out.reshape(kv_cache.shape)


def solution(mesh):
    placed = (
        P(("dp", "tp"), None),
        P(),
        P(),
        P(None, None, "tp"),
        P(None, "tp"),
        P("tp", None),
        P(),
        P(None, "dp", None, "tp"),
        P("dp", None),
        P("dp"),
    )
    return jax.shard_map(
        body,
        mesh=mesh,
        in_specs=placed,
        out_specs=(P(("dp", "tp"), None), P(None, "dp", None, "tp")),
        check_vma=False,
    )
```

```python
import functools

import jax
import jax.numpy as jnp
from jax import lax
from jax.experimental import pallas as pl
from jax.experimental.pallas import tpu as pltpu
from jax.sharding import PartitionSpec as P

HD = 128
EPS = 1e-05
MESH = pl.DeviceIdType.MESH
RINGS = 4
SUBS = 3
N = 16
ROWS = 80
CW = 512
QW = SUBS * CW
D = RINGS * QW
LEN = N * ROWS
F = 384
HEADS = F // HD
BQ = 320
BATCH = 4
PAGE = 128
PAGES = LEN // PAGE
SLOTS = 12
HC = D // 2
PR = F // 8
KX = 4 * F
CHUNKS = 12
LAG = 4
QB = 256
PIECES = ((0, 320, 0), (320, 640, 1), (640, 960, 2), (960, 1024, 3), (1024, 1280, 3))
SPAN = 4
FORWARD_AT = 4
SCALE2 = 1.4426950408889634 / (HD ** 0.5)


def ring_tp(ring, pos):
    a = lax.div(pos, 4)
    b = lax.rem(lax.rem(pos, 4) - a + 4, 4)
    return jnp.where(ring < 2, a * 4 + b, b * 4 + a)


def my_pos(ring, z, x):
    t = lax.rem(z + x, 4)
    return jnp.where(ring < 2, 4 * z + t, 4 * x + t)


def behind(ring, pos, k):
    up = lax.rem(ring, 2)
    return lax.rem(jnp.where(up == 0, pos + N - k, pos + k), N)


def main_kernel(
    len_ref, tok_hbm, gain_hbm, shift_hbm, w_hbm, bq_hbm, wo_hbm, bo_hbm,
    out_ref, kv_hbm, g_hbm,
    ag, w, acc, qkv, att, wx, gat, psend, prec, out,
    tok_ref, gain_ref, shift_ref, bq_ref, bo_ref, in_sem,
    ag_send, ag_recv, w_sem, kv_sem, out_sem,
    g_send, g1_recv, g2_recv, gy_recv, gf_recv, gd_recv,
    l_sem, az_send, az_recv, ax_send, ax_recv, p_send, p0_recv, p_recv,
):
    tp = lax.axis_index("tp")
    dp = lax.axis_index("dp")
    z = lax.div(tp, 4)
    x = lax.rem(tp, 4)
    y = lax.div(dp, 2)
    core = lax.rem(dp, 2)
    pos = [my_pos(jnp.int32(r), z, x) for r in range(RINGS)]
    nxt = [ring_tp(jnp.int32(r), behind(jnp.int32(r), pos[r], N - 1)) for r in range(RINGS)]

    def along(axis, j):
        if axis == 0:
            return {"tp": z * 4 + lax.rem(x + j, 4)}
        return {"tp": lax.rem(z + j, 4) * 4 + x}

    def along_y(j):
        return {"dp": lax.rem(y + j, 4) * 2 + core}

    sibling = {"dp": y * 2 + 1 - core}

    barrier = pltpu.get_barrier_semaphore()
    peers = [along(a, j) for a in range(2) for j in (1, 2, 3)] + [along_y(1), along_y(3), sibling]
    for peer in peers:
        pl.semaphore_signal(barrier, inc=1, device_id=peer, device_id_type=MESH)

    inputs = [
        pltpu.make_async_copy(src, dst, in_sem.at[i])
        for i, (src, dst) in enumerate(
            (
                (tok_hbm, tok_ref), (gain_hbm, gain_ref), (shift_hbm, shift_ref),
                (bq_hbm, bq_ref), (bo_hbm, bo_ref),
            )
        )
    ]
    for copy in inputs:
        copy.start()

    w_copies = [
        pltpu.make_async_copy(w_hbm.at[c], w.at[:, pl.ds(c * F, F)], w_sem) for c in range(3)
    ]
    for copy in w_copies:
        copy.start()
    pl.semaphore_wait(barrier, len(peers))

    def remote(src, dst, send_sem, recv_sem, device):
        return pltpu.make_async_remote_copy(
            src_ref=src, dst_ref=dst, send_sem=send_sem, recv_sem=recv_sem,
            device_id=device, device_id_type=MESH,
        )

    piece = pl.ds(pl.multiple_of((core * 4 + y) * PR, PR), PR)

    def g1_copy(axis, j):
        return remote(
            wo_hbm.at[piece, pl.ds(axis * HC, HC)], g_hbm.at[axis, 3 - j, piece],
            g_send.at[0], g1_recv.at[axis, j // 2], along(axis, j),
        )

    def g2_copy(axis, j):
        k = 4 - j
        cols = pl.ds(0 if j == 1 else HC // 2, HC // 2)
        return remote(
            g_hbm.at[axis, k - 1, piece, cols], g_hbm.at[axis, 1, piece, cols],
            g_send.at[1], g2_recv.at[axis, j // 2], along(axis, j),
        )

    for axis in range(2):
        for j in (1, 3):
            g1_copy(axis, j).start()

    def norm_rows(i, carry):
        rows = pl.ds(pl.multiple_of(i * 16, 16), 16)
        v = tok_ref[rows, :].astype(jnp.float32)
        center = jnp.mean(v, axis=-1, keepdims=True)
        v = v - center
        spread = jnp.mean(v * v, axis=-1, keepdims=True)
        v = (v * lax.rsqrt(spread + EPS) * gain_ref[...] + shift_ref[...]).astype(jnp.bfloat16)
        for r in range(RINGS):
            for c in range(SUBS):
                ag[r, c, rows, :] = v[:, r * QW + c * CW : r * QW + (c + 1) * CW]
        return carry

    for copy in inputs:
        copy.wait()
    lax.fori_loop(0, ROWS // 16, norm_rows, 0)

    def slot(s):
        if isinstance(s, int):
            return pl.ds(s * ROWS, ROWS)
        return pl.ds(pl.multiple_of(s * ROWS, 16), ROWS)

    def ag_copy(r, c, s):
        return remote(
            ag.at[r, c, slot(s)], ag.at[r, c, slot(s + 1)],
            ag_send.at[r, c], ag_recv.at[r, c, lax.rem(s + 1, SPAN)], {"tp": nxt[r]},
        )

    def ag_arrived(r, c, s):
        return remote(
            ag.at[r, c, slot(s)], ag.at[r, c, slot(s)],
            ag_send.at[r, c], ag_recv.at[r, c, lax.rem(s, SPAN)], {"tp": nxt[r]},
        )

    for r in range(RINGS):
        ag_copy(r, 0, 0).start()
    for j in (1, 3):
        for axis in range(2):
            g1_copy(axis, j).wait_recv()
            g2_copy(axis, j).start()
    for c in range(1, SUBS):
        for r in range(RINGS):
            ag_copy(r, c, 0).start()

    for c in range(3):
        acc[:, c * F : (c + 1) * F] = jnp.broadcast_to(bq_ref[c : c + 1, :], (LEN, F))
    pltpu.make_async_copy(w, w, w_sem).wait()

    def gy_copy(axis, k, j):
        return remote(
            g_hbm.at[axis, k - 1, piece], g_hbm.at[axis, k - 1, piece],
            g_send.at[2 + axis], gy_recv.at[axis, k - 1, j // 2], along_y(j),
        )

    def gf_copy(axis, k):
        j = 1 if axis == 0 else 3
        src = pl.ds(pl.multiple_of((core * 4 + lax.rem(y + 4 - j, 4)) * PR, PR), PR)
        return remote(
            g_hbm.at[axis, k - 1, src], g_hbm.at[axis, k - 1, src],
            g_send.at[4], gf_recv.at[axis, k - 1], along_y(j),
        )

    for k in (1, 3, 2):
        if k == 2:
            for axis in range(2):
                for j in (1, 3):
                    g2_copy(axis, j).wait_recv()
        for axis in range(2):
            gy_copy(axis, k, 1 if axis == 0 else 3).start()
    for k in (1, 3, 2):
        for axis in range(2):
            gy_copy(axis, k, 3 if axis == 0 else 1).start()

    def unit(first, count, r, subs, cols):
        home = jnp.where(r < 2, 4 * z, 4 * x) + lax.rem(z + x, 4)
        rows = pl.ds(pl.multiple_of(first * ROWS, 16), count * ROWS)
        for lo, hi in cols:
            res = None
            for c in subs:
                wrow = pl.ds(pl.multiple_of(r * QW + c * CW, CW), CW)
                part = jnp.dot(ag[r, c, rows, :], w[wrow, lo:hi], preferred_element_type=jnp.float32)
                res = part if res is None else res + part
            for i in range(count):
                src = ring_tp(r, behind(r, home, first + i))
                to = pl.ds(pl.multiple_of(src * ROWS, 16), ROWS)
                acc[to, lo:hi] += res[i * ROWS : (i + 1) * ROWS]

    halves, whole = ((0, 640), (640, 1152)), ((0, 1152),)

    mine = pl.ds(pl.multiple_of(core * (4 * PR), 4 * PR), 4 * PR)

    def gd_copy(axis, k):
        return remote(
            g_hbm.at[axis, k - 1, mine], g_hbm.at[axis, k - 1, mine],
            g_send.at[5], gd_recv.at[axis, k - 1], sibling,
        )

    blocks = [(axis, k) for axis in range(2) for k in (1, 2, 3)]

    def ag_step(s, carry):
        first = jnp.where(s < 12, s - 4, 2 * s - 16)
        count = jnp.where(s < 4, 0, jnp.where(s < 12, 1, jnp.where(s < 14, 2, 0)))
        for c in range(SUBS):
            for r in range(RINGS):
                ag_arrived(r, c, s).wait_recv()
                ag_copy(r, c, s - 1).wait_send()
                ag_copy(r, c, s).start()

            def four(u, carry, c=c):
                unit(lax.div(u, RINGS) * 4, 4, lax.rem(u, RINGS), (c,), halves)
                return carry

            lax.fori_loop(first, first + count, four, 0)

        for i, k in enumerate((1, 3, 2)):

            @pl.when(s == FORWARD_AT + i)
            def _():
                for axis in range(2):
                    gy_copy(axis, k, 1 if axis == 0 else 3).wait_recv()
                    gf_copy(axis, k).start()

        @pl.when(s == 13)
        def _():
            for axis, k in blocks:
                gy_copy(axis, k, 3 if axis == 0 else 1).wait_recv()
                gf_copy(axis, k).wait_recv()
                gd_copy(axis, k).start()

        return carry

    lax.fori_loop(1, N - 1, ag_step, 0)

    def two(first):
        def step(r, carry):
            unit(first, 2, r, (0, 1, 2), whole)
            return carry

        lax.fori_loop(0, RINGS, step, 0)

    two(12)
    for c in range(SUBS):
        for r in range(RINGS):
            ag_arrived(r, c, N - 1).wait_recv()
            ag_copy(r, c, N - 2).wait_send()
    two(14)

    def to_bf16(i, carry):
        rows = pl.ds(pl.multiple_of(i * 64, 64), 64)
        qkv[rows, :] = acc[rows, :].astype(jnp.bfloat16)
        return carry

    lax.fori_loop(0, LEN // 64, to_bf16, 0)

    kv_copy = pltpu.make_async_copy(qkv.at[:, pl.ds(F, 2 * F)], kv_hbm, kv_sem)
    kv_copy.start()

    def home_of(n):
        if n < 8:
            return w, (n // 2) * KX, (n % 2) * CW
        return wx, 0, (n - 8) * CW

    def load(n, k):
        axis, m = n % 2, n // 2
        ref, row, col = home_of(n)
        if k == 0:
            src = wo_hbm.at[:, pl.ds(axis * HC + m * CW, CW)]
        else:
            src = g_hbm.at[axis, k - 1, :, pl.ds(m * CW, CW)]
        return pltpu.make_async_copy(src, ref.at[pl.ds(row + k * F, F), pl.ds(col, CW)], l_sem.at[n])

    def loaded(n):
        ref, row, col = home_of(n)
        chunk = ref.at[pl.ds(row, KX), pl.ds(col, CW)]
        return pltpu.make_async_copy(chunk, chunk, l_sem.at[n])

    last = len_ref[0] - 1

    def az_copy(h, lo, hi, qi, k):
        src = att.at[pl.ds(lo, hi - lo), pl.ds(h * HD, HD)]
        there = pl.ds(pl.multiple_of(k * F + h * HD, HD), HD)
        return remote(
            src, gat.at[1, pl.ds(lo - qi * BQ, hi - lo), there],
            az_send.at[h], az_recv.at[h, k - 1], {"tp": qi * 4 + x},
        )

    def ax_copy(h, qi, j):
        block = pl.ds(pl.multiple_of((4 * qi + lax.rem(x + j, 4)) * ROWS, 16), ROWS)
        src = att.at[block, pl.ds(h * HD, HD)]
        there = pl.ds((4 - j) * F + h * HD, HD)
        return remote(
            src, gat.at[0, pl.ds(qi * ROWS, ROWS), there], ax_send.at[h], ax_recv.at[h, 3 - j], along(0, j)
        )

    def a_all(axis, h, k):
        part = gat.at[axis, :, pl.ds(h * HD, HD)]
        sends, recvs = ((ax_send, ax_recv), (az_send, az_recv))[axis]
        return remote(part, part, sends.at[h], recvs.at[h, k - 1], along(axis, k))

    def a_sent(axis, h):
        part = gat.at[axis, :, pl.ds(0, 3 * HD)]
        return remote(part, part, (ax_send, az_send)[axis].at[h], ax_recv.at[h, 0], along(0, 1))

    for h in range(HEADS):
        q0, k0, v0 = h * HD, F + h * HD, 2 * F + h * HD
        for row in range(0, LEN, QB):
            kv = row + QB
            free = min(row, LEN // 2)
            q = qkv[row:kv, q0 : q0 + HD]
            k = qkv[0:kv, k0 : k0 + HD]
            v = qkv[0:kv, v0 : v0 + HD]
            sc = lax.dot_general(q, k, (((1,), (1,)), ((), ())), preferred_element_type=jnp.float32)
            limit = jnp.minimum(lax.broadcasted_iota(jnp.int32, (QB, 1), 0) + row, last)
            key = lax.broadcasted_iota(jnp.int32, (QB, kv - free), 1) + free
            masked = jnp.where(key <= limit, sc[:, free:], -1e30)
            sc = jnp.concatenate([sc[:, :free], masked], axis=1) if free else masked
            top = jnp.max(sc, axis=-1, keepdims=True)
            e = jnp.exp2((sc - top) * SCALE2)
            inv = 1.0 / jnp.sum(e, axis=-1, keepdims=True)
            p = (e * inv).astype(jnp.bfloat16)
            o = jnp.dot(p, v, preferred_element_type=jnp.float32)
            att[row:kv, q0 : q0 + HD] = o.astype(jnp.bfloat16)
            for lo, hi, qi in PIECES:
                if row < hi <= kv:

                    @pl.when(z != qi)
                    def _():
                        az_copy(h, lo, hi, qi, lax.rem(z - qi + 4, 4)).start()

                    if hi == (qi + 1) * BQ:
                        for j in (2, 1, 3):
                            ax_copy(h, qi, j).start()
        if h == 1:
            for axis, k in blocks:
                gd_copy(axis, k).wait_recv()
            for n in range(CHUNKS):
                for k in range(4):
                    load(n, k).start()

    for b in range(4):
        gat[0, b * ROWS : (b + 1) * ROWS, 0:F] = att[pl.ds(pl.multiple_of((4 * b + x) * ROWS, 16), ROWS), :]
    gat[1, :, 0:F] = att[pl.ds(pl.multiple_of(z * BQ, 64), BQ), :]

    def out_copy(n):
        lo = (n % 2) * HC + (n // 2) * CW
        return pltpu.make_async_copy(out.at[n], out_ref.at[:, pl.ds(lo, CW)], out_sem.at[n])

    def p_copy(n, what):
        axis, ahead = 1 - n % 2, (1 if (n // 2) % 2 == 0 else 3)
        here = x if axis == 0 else z
        j = (ahead, ahead, 4 - ahead)[what]
        block = lax.rem(here + (2 if what == 0 else j), 4)
        return remote(
            psend.at[n, block], prec.at[n, what], p_send.at[n],
            p0_recv.at[n] if what == 0 else p_recv.at[n], along(axis, j),
        )

    def p_all(n, count):
        part = prec.at[n, pl.ds(0, count)]
        return remote(part, part, p_send.at[n], p_recv.at[n], along(0, 1))

    def p_add(n):
        axis, ahead = 1 - n % 2, (1 if (n // 2) % 2 == 0 else 3)
        block = lax.rem((x if axis == 0 else z) + ahead, 4)
        p_copy(n, 0).wait_recv()
        both = psend[n, block].astype(jnp.float32) + prec[n, 0].astype(jnp.float32)
        psend[n, block] = both.astype(jnp.bfloat16)
        p_copy(n, 1).start()

    for n in range(CHUNKS):
        ref, row, col = home_of(n)
        if n < 2:
            for h in range(HEADS):
                for k in (1, 2, 3):
                    a_all(n, h, k).wait_recv()
        loaded(n).wait()
        res = jnp.dot(gat[n % 2], ref[row : row + KX, col : col + CW], preferred_element_type=jnp.float32)
        psend[n] = res.astype(jnp.bfloat16).reshape(4, ROWS, CW)
        p_copy(n, 0).start()
        p_copy(n, 2).start()
        if n >= LAG:
            p_add(n - LAG)
    for n in range(CHUNKS - LAG, CHUNKS):
        p_add(n)

    for n in range(CHUNKS):
        here = z if n % 2 == 0 else x
        lo = (n % 2) * HC + (n // 2) * CW
        total = psend[n, here].astype(jnp.float32) + bo_ref[:, lo : lo + CW]
        p_all(n, 2).wait_recv()
        total += prec[n, 1].astype(jnp.float32) + prec[n, 2].astype(jnp.float32)
        out[n] = total.astype(jnp.bfloat16)
        out_copy(n).start()

    for n in range(CHUNKS):
        p_all(n, 3).wait_send()
    for i, sent in enumerate(
        (
            g_hbm.at[0, 0, pl.ds(0, 4 * PR)],
            g_hbm.at[0, 0, pl.ds(0, 2 * PR)],
            g_hbm.at[0, 0, pl.ds(0, 6 * PR)],
            g_hbm.at[0, 0, pl.ds(0, 6 * PR)],
            g_hbm.at[0, 0, pl.ds(0, 6 * PR)],
            g_hbm.at[0],
        )
    ):
        remote(sent, sent, g_send.at[i], gd_recv.at[0, 0], sibling).wait_send()
    for h in range(HEADS):
        for axis in range(2):
            a_sent(axis, h).wait_send()
    for n in range(CHUNKS):
        out_copy(n).wait()
    kv_copy.wait()


def finish_kernel(page_ref, len_ref, part_hbm, new_hbm, old_hbm, out_hbm, kv_hbm, part, new, kv, in_sem, out_sem):
    load = pltpu.make_async_copy(part_hbm, part, in_sem.at[SLOTS])
    load.start()

    def rows_of(i):
        return pl.ds(pl.multiple_of(i * PAGE, PAGE), PAGE)

    def old_copy(i):
        return pltpu.make_async_copy(old_hbm.at[:, rows_of(i)], kv.at[:, rows_of(i)], in_sem.at[i])

    def kv_copy(i):
        return pltpu.make_async_copy(kv.at[:, rows_of(i)], kv_hbm.at[:, rows_of(i)], out_sem.at[i])

    def new_copy(page):
        return pltpu.make_async_copy(new_hbm.at[rows_of(page)], new, in_sem.at[SLOTS + 1])

    used = []
    for i in range(SLOTS):
        page = jnp.int32(-1)
        for p in range(PAGES):
            page = jnp.where(page_ref[0, p] == i, p, page)
        count = jnp.where(page < 0, 0, jnp.clip(len_ref[0] - page * PAGE, 0, PAGE))
        page = jnp.maximum(page, 0)
        used.append((page, count))

        @pl.when(count == PAGE)
        def _():
            for c in range(2):
                pltpu.make_async_copy(
                    new_hbm.at[rows_of(page), pl.ds(c * F, F)], kv.at[c, rows_of(i)], in_sem.at[i]
                ).start()

        @pl.when(count < PAGE)
        def _():
            old_copy(i).start()

        @pl.when((count > 0) & (count < PAGE))
        def _():
            new_copy(page).start()

    store = pltpu.make_async_copy(part, out_hbm, out_sem.at[SLOTS])
    load.wait()
    store.start()
    for i, (page, count) in enumerate(used):
        old_copy(i).wait()

        @pl.when((count > 0) & (count < PAGE))
        def _():
            new_copy(page).wait()
            written = lax.broadcasted_iota(jnp.int32, (PAGE, 1), 0) < count
            for c in range(2):
                rows = pl.ds(i * PAGE, PAGE)
                kv[c, rows, :] = jnp.where(written, new[:, c * F : (c + 1) * F], kv[c, rows, :])

        kv_copy(i).start()
    for i in range(SLOTS):
        kv_copy(i).wait()
    store.wait()


def body(tokens, ln_gain, ln_bias, w_qkv, b_qkv, w_out, b_out, kv_cache, page_table, lengths):
    anym = pl.BlockSpec(memory_space=pl.ANY)
    smem = pl.BlockSpec(memory_space=pltpu.SMEM)
    dma = pltpu.SemaphoreType.DMA
    part, kv_new, _ = pl.pallas_call(
        main_kernel,
        out_shape=(
            jax.ShapeDtypeStruct((ROWS, D), jnp.bfloat16),
            jax.ShapeDtypeStruct((LEN, 2 * F), jnp.bfloat16),
            jax.ShapeDtypeStruct((2, 3, F, HC), jnp.bfloat16),
        ),
        in_specs=[smem] + [anym] * 7,
        out_specs=(anym, anym, anym),
        scratch_shapes=[
            pltpu.VMEM((RINGS, SUBS, LEN, CW), jnp.bfloat16),
            pltpu.VMEM((D, 3 * F), jnp.bfloat16),
            pltpu.VMEM((LEN, 3 * F), jnp.float32),
            pltpu.VMEM((LEN, 3 * F), jnp.bfloat16),
            pltpu.VMEM((LEN, F), jnp.bfloat16),
            pltpu.VMEM((KX, 4 * CW), jnp.bfloat16),
            pltpu.VMEM((2, BQ, KX), jnp.bfloat16),
            pltpu.VMEM((CHUNKS, 4, ROWS, CW), jnp.bfloat16),
            pltpu.VMEM((CHUNKS, 3, ROWS, CW), jnp.bfloat16),
            pltpu.VMEM((CHUNKS, ROWS, CW), jnp.bfloat16),
            pltpu.VMEM((ROWS, D), jnp.bfloat16),
            pltpu.VMEM((1, D), jnp.float32),
            pltpu.VMEM((1, D), jnp.float32),
            pltpu.VMEM((3, F), jnp.float32),
            pltpu.VMEM((1, D), jnp.float32),
            dma((5,)),
            dma((RINGS, SUBS)),
            dma((RINGS, SUBS, SPAN)),
            dma,
            dma,
            dma((CHUNKS,)),
            dma((6,)),
            dma((2, 2)),
            dma((2, 2)),
            dma((2, 3, 2)),
            dma((2, 3)),
            dma((2, 3)),
            dma((CHUNKS,)),
            dma((HEADS,)),
            dma((HEADS, 3)),
            dma((HEADS,)),
            dma((HEADS, 3)),
            dma((CHUNKS,)),
            dma((CHUNKS,)),
            dma((CHUNKS,)),
        ],
        compiler_params=pltpu.CompilerParams(
            collective_id=0, has_side_effects=True, vmem_limit_bytes=67043328
        ),
        name="sublayer",
    )(
        lengths,
        tokens,
        ln_gain.reshape(1, D),
        ln_bias.reshape(1, D),
        jnp.transpose(w_qkv, (1, 0, 2)),
        b_qkv,
        w_out,
        b_out.reshape(1, D),
    )
    out, kv_out = pl.pallas_call(
        finish_kernel,
        out_shape=(
            jax.ShapeDtypeStruct((ROWS, D), jnp.bfloat16),
            jax.ShapeDtypeStruct((2, SLOTS * PAGE, F), jnp.bfloat16),
        ),
        in_specs=[smem, smem, anym, anym, anym],
        out_specs=(anym, anym),
        scratch_shapes=[
            pltpu.VMEM((ROWS, D), jnp.bfloat16),
            pltpu.VMEM((PAGE, 2 * F), jnp.bfloat16),
            pltpu.VMEM((2, SLOTS * PAGE, F), jnp.bfloat16),
            dma((SLOTS + 2,)),
            dma((SLOTS + 1,)),
        ],
        name="finish",
    )(page_table, lengths, part, kv_new, kv_cache.reshape(2, SLOTS * PAGE, F))
    return out, kv_out.reshape(kv_cache.shape)


def solution(mesh):
    placed = (
        P(("dp", "tp"), None),
        P(),
        P(),
        P(None, None, "tp"),
        P(None, "tp"),
        P("tp", None),
        P(),
        P(None, "dp", None, "tp"),
        P("dp", None),
        P("dp"),
    )
    return jax.shard_map(
        body,
        mesh=mesh,
        in_specs=placed,
        out_specs=(P(("dp", "tp"), None), P(None, "dp", None, "tp")),
        check_vma=False,
    )
```
